32 devices in a mesh: lon: 8 (over y, x, core), lat: 4 (over z).
Axes of the slice: x: 2, y: 2, z: 4, core: 2. Of those that a mesh axis runs over, the one named last changes fastest.
Arguments:
- fields: bfloat16 [4, 128, 32, 1024], P(None, None, 'lat', 'lon'), may hold values from -12 to 12
- bracket: int32 [32, 32, 1024], P(None, 'lat', 'lon'), may hold values from 0 to 126, as said below
- fraction: bfloat16 [32, 32, 1024], P(None, 'lat', 'lon'), may hold values from 0 to 1
Outputs:
- on_pressure: bfloat16 [4, 32, 32, 1024], P(None, None, ('lat', 'lon'))
- zonal_mean: float32 [4, 32, 32], P(None, None, ('lat', 'lon'))
- meridional: float32 [4, 32, 32], P(None, None, ('lat', 'lon'))
The draws below stay inside these ranges and needn't reach their ends.
Inputs may be any that keep to these rules, and one draw needn't show every extreme that they name: bracket[p, r, c] - min(p * 4, 112) lies in 0 to 14 for every column, and each of these offsets occurs.
All inputs are finite; a program needn't handle non-finite values.
Results may differ from the reference program's by a relative error of at most 0.0012.
Values may be sent and summed in bfloat16 or wider, within the bound.
No kernel may reach another device: no remote copies, remote signals or barrier semaphores. Data moves between devices by JAX's collectives and lax.ppermute only.
A program may use at most 128 MiB of HBM per device.

```python
import jax
import jax.numpy as jnp
from jax import lax

VARS = 4
LEV = 128
PLEV = 32
WINDOW = 16
NLAT = 32
NLON = 1024


def draw_fields(key, part):
    key_noise = jax.random.fold_in(key, 11)
    key_offset = jax.random.fold_in(key, 12)
    noise_part = jnp.clip(jax.random.normal(key_noise, (VARS, LEV, NLAT, NLON), jnp.float32), -4.0, 4.0)
    offset = jax.random.uniform(key_offset, (VARS, LEV, NLAT, 1), jnp.float32, -4.0, 4.0)
    values = noise_part + offset
    return values.astype(jnp.bfloat16)


def draw_bracket(key, part):
    key_offset = jax.random.fold_in(key, 21)
    level_step = LEV // PLEV
    pressure_index = jnp.arange(PLEV, dtype=jnp.int32).reshape(PLEV, 1, 1)
    window_base = jnp.minimum(pressure_index * level_step, LEV - WINDOW)
    offsets = jax.random.randint(key_offset, (PLEV, NLAT, NLON), 0, WINDOW - 1, dtype=jnp.int32)
    return (window_base + offsets).astype(jnp.int32)


def shard_levels(key, shape, cuts, low, largest):
    def one(dim, blocks):
        steps = jax.random.uniform(jax.random.fold_in(jax.random.fold_in(key, 6), dim), (blocks,), jnp.float32, low / len(cuts), largest / len(cuts))
        return jnp.repeat(jnp.exp(steps), shape[dim] // blocks).reshape((-1,) + (1,) * (len(shape) - dim - 1))

    level = one(*cuts[0])
    for cut in cuts[1:]:
        level = level * one(*cut)
    return level


def setup_inputs(seed: int = 0) -> dict:
    streams_of = jax.random.split(jax.random.key(seed), 4)
    return {
        "fields": draw_fields(jax.random.fold_in(streams_of[3], 71), 0),
        "bracket": draw_bracket(jax.random.fold_in(streams_of[3], 71), 0),
        "fraction": jnp.clip(1.0 * jax.random.uniform(streams_of[2], (PLEV, NLAT, NLON), jnp.float32) ** shard_levels(streams_of[2], (PLEV, NLAT, NLON), ((1, 4), (2, 8)), -0.2, 0.2), 0.0, 1.0).astype(jnp.bfloat16),
    }


def interpolate(block, bracket, fraction):
    index = jnp.broadcast_to(bracket[None], (block.shape[0],) + bracket.shape)
    lower_level = jnp.take_along_axis(block, index, axis=1).astype(jnp.float32)
    upper_level = jnp.take_along_axis(block, index + 1, axis=1).astype(jnp.float32)
    weight = fraction.astype(jnp.float32)[None]
    return (lower_level + weight * (upper_level - lower_level)).astype(jnp.bfloat16)


def reference(fields, bracket, fraction):
    on_pressure = lax.map(lambda single: interpolate(single[None], bracket, fraction)[0], fields)
    zonal_mean = jnp.sum(on_pressure.astype(jnp.float32), axis=3) / jnp.float32(NLON)
    centered = 0.5 * (zonal_mean[:, :, 2:] - zonal_mean[:, :, :-2])
    first_row = zonal_mean[:, :, 1:2] - zonal_mean[:, :, 0:1]
    last_row = zonal_mean[:, :, -1:] - zonal_mean[:, :, -2:-1]
    meridional = jnp.concatenate([first_row, centered, last_row], axis=2)
    return on_pressure, zonal_mean, meridional
```

```python
import functools

import jax
import jax.numpy as jnp
from jax import lax
from jax.experimental import pallas as pl
from jax.experimental.pallas import tpu as pltpu
from jax.sharding import PartitionSpec as P

WINDOW = 16
SUBLANES = 8
bf16, f32 = jnp.bfloat16, jnp.float32
VMEM = pl.BlockSpec(memory_space=pltpu.VMEM)


def interpolate_kernel(fields, bracket, fraction, payload, flat, totals, *, levels):
    groups, variables = fields.shape[:2]
    plev = bracket.shape[1]
    pairs = variables * plev
    step = levels // plev

    def one_group(group):
        for p in range(plev):
            base = min(p * step, levels - WINDOW)
            offset = bracket[group, p] - base
            index = jnp.concatenate([(offset + 1) >> 1, offset >> 1], 0).astype(f32).astype(bf16)
            high = index >= bf16(4)
            index = jnp.where(high, index - bf16(4), index)
            mid = index >= bf16(2)
            index = jnp.where(mid, index - bf16(2), index)
            low = index >= bf16(1)
            is_odd = (offset & 1) == 1
            weight = fraction[group, p].astype(f32)
            weight = jnp.where(is_odd, -weight, weight)
            for v in range(variables):
                w = [fields[group, v, base // 2 + k] for k in range(WINDOW // 2)]
                w = [jnp.where(low, w[k + 1], w[k]) for k in (0, 2, 4, 6)]
                w = [jnp.where(mid, w[k + 1], w[k]) for k in (0, 2)]
                picked = jnp.where(high, w[1], w[0]).astype(f32)
                even, odd = picked[:SUBLANES], picked[SUBLANES:]
                value = jnp.where(is_odd, odd, even) + weight * (odd - even)
                flat[pl.ds(v * plev + p, SUBLANES, stride=pairs), :] = value
        ones = jnp.ones((SUBLANES, flat.shape[1]), bf16)
        sums = []
        for r in range(SUBLANES):
            block = flat[r * pairs : (r + 1) * pairs, :].astype(bf16)
            payload[group * SUBLANES + r, :pairs, :] = block
            total = lax.dot_general(ones, block, (((1,), (1,)), ((), ())), preferred_element_type=f32)
            sums.append(total[:1])
        totals[group] = jnp.concatenate(sums, 0)

    if groups == 1:
        one_group(0)
    else:
        pl.loop(0, groups)(one_group)
    sums = totals[...].reshape(groups * SUBLANES, pairs)
    main = sums.astype(bf16)
    both = jnp.concatenate([main, (sums - main.astype(f32)).astype(bf16)], 0)
    for r in range(groups * SUBLANES):
        payload[r, pairs:, :] = both


def interpolate(fields, bracket, fraction):
    variables, levels, rows, columns = fields.shape
    plev = bracket.shape[0]
    groups = rows // SUBLANES
    pairs = variables * plev
    assert rows % SUBLANES == 0 and levels % 2 == 0 and pairs == columns
    grouped = fields.reshape(variables, levels, groups, SUBLANES, columns).transpose(2, 0, 1, 3, 4)
    grouped = grouped.reshape(groups, variables, levels // 2, 2 * SUBLANES, columns)
    bracket = bracket.reshape(plev, groups, SUBLANES, columns).transpose(1, 0, 2, 3)
    fraction = fraction.reshape(plev, groups, SUBLANES, columns).transpose(1, 0, 2, 3)
    return pl.pallas_call(
        functools.partial(interpolate_kernel, levels=levels),
        out_shape=jax.ShapeDtypeStruct((rows, pairs + 2 * rows, columns), bf16),
        in_specs=[VMEM] * 3,
        out_specs=VMEM,
        scratch_shapes=[
            pltpu.VMEM((SUBLANES * pairs, columns), f32),
            pltpu.VMEM((groups, SUBLANES, pairs), f32),
        ],
        name="interpolate",
    )(grouped, bracket, fraction)


def lay_kernel(received, whole, sem):
    parts, _, columns = received.shape
    pairs = whole.shape[0]
    copies = [
        pltpu.make_async_copy(
            received.at[j, :pairs], whole.at[:, j * columns : (j + 1) * columns], sem.at[j]
        )
        for j in range(parts)
    ]
    for copy in copies:
        copy.start()
    for copy in copies:
        copy.wait()


def lay(received, pairs):
    parts, _, columns = received.shape
    return pl.pallas_call(
        lay_kernel,
        out_shape=jax.ShapeDtypeStruct((pairs, parts * columns), bf16),
        in_specs=[pl.BlockSpec(memory_space=pl.ANY)],
        out_specs=pl.BlockSpec(memory_space=pl.ANY),
        scratch_shapes=[pltpu.SemaphoreType.DMA((parts,))],
        compiler_params=pltpu.CompilerParams(vmem_limit_bytes=1 << 20),
        cost_estimate=pl.CostEstimate(
            flops=2 * pairs * parts * columns * 1024, bytes_accessed=4 * pairs * parts * columns, transcendentals=0
        ),
        name="lay",
    )(received)


def shards(fields, bracket, fraction):
    variables, _, rows, columns = fields.shape
    plev = bracket.shape[0]
    pairs = variables * plev
    lon_count, lat_count = lax.axis_size("lon"), lax.axis_size("lat")
    lon_place, lat_place = lax.axis_index("lon"), lax.axis_index("lat")
    assert rows == lon_count

    payload = interpolate(fields, bracket, fraction)
    received = lax.all_to_all(payload, "lon", split_axis=0, concat_axis=0, tiled=True)

    sums = jnp.sum(received[:, pairs:].astype(f32), 0)
    means = (sums[:rows] + sums[rows:]) / f32(lon_count * columns)
    first_place, last_place = lon_place == 0, lon_place == lon_count - 1

    edge = jnp.where(first_place, means[rows - 1], means[0])
    route = [(b, b + 1) for b in range(lat_count - 1)]
    along = [(0 * lat_count + s, 0 * lat_count + t) for s, t in route]
    along += [((lon_count - 1) * lat_count + t, (lon_count - 1) * lat_count + s) for s, t in route]
    beyond = lax.ppermute(edge, ("lon", "lat"), along)

    on_pressure = lay(received, pairs)

    own = lax.dynamic_index_in_dim(means, lon_place, 0, False)
    below = lax.dynamic_index_in_dim(means, jnp.maximum(lon_place - 1, 0), 0, False)
    above = lax.dynamic_index_in_dim(means, jnp.minimum(lon_place + 1, rows - 1), 0, False)
    below = jnp.where(first_place, beyond, below)
    above = jnp.where(last_place, beyond, above)
    first_row = first_place & (lat_place == 0)
    last_row = last_place & (lat_place == lat_count - 1)
    meridional = jnp.where(
        first_row, above - own, jnp.where(last_row, own - below, 0.5 * (above - below))
    )
    return (
        on_pressure.reshape(variables, plev, 1, lon_count * columns),
        own.reshape(variables, plev, 1),
        meridional.reshape(variables, plev, 1),
    )


def solution(mesh):
    return jax.shard_map(
        shards,
        mesh=mesh,
        in_specs=(P(None, None, "lat", "lon"), P(None, "lat", "lon"), P(None, "lat", "lon")),
        out_specs=(
            P(None, None, ("lat", "lon"), None),
            P(None, None, ("lat", "lon")),
            P(None, None, ("lat", "lon")),
        ),
        check_vma=False,
    )
```

```python
import functools

import jax
import jax.numpy as jnp
from jax import lax
from jax.experimental import pallas as pl
from jax.experimental.pallas import tpu as pltpu
from jax.sharding import PartitionSpec as P

WINDOW = 16
SUBLANES = 8
bf16, f32 = jnp.bfloat16, jnp.float32
VMEM = pl.BlockSpec(memory_space=pltpu.VMEM)


def interpolate_kernel(fields, bracket, fraction, payload, flat, totals, *, levels):
    groups, variables = fields.shape[:2]
    plev = bracket.shape[1]
    pairs = variables * plev
    step = levels // plev

    def one_group(group):
        for p in range(plev):
            base = min(p * step, levels - WINDOW)
            offset = bracket[group, p] - base
            index = jnp.concatenate([(offset + 1) >> 1, offset >> 1], 0).astype(f32).astype(bf16)
            high = index >= bf16(4)
            index = jnp.where(high, index - bf16(4), index)
            mid = index >= bf16(2)
            index = jnp.where(mid, index - bf16(2), index)
            low = index >= bf16(1)
            is_odd = (offset & 1) == 1
            weight = fraction[group, p].astype(f32)
            weight = jnp.where(is_odd, -weight, weight)
            for v in range(variables):
                w = [fields[group, v, base // 2 + k] for k in range(WINDOW // 2)]
                w = [jnp.where(low, w[k + 1], w[k]) for k in (0, 2, 4, 6)]
                w = [jnp.where(mid, w[k + 1], w[k]) for k in (0, 2)]
                picked = jnp.where(high, w[1], w[0]).astype(f32)
                even, odd = picked[:SUBLANES], picked[SUBLANES:]
                value = jnp.where(is_odd, odd, even) + weight * (odd - even)
                flat[pl.ds(v * plev + p, SUBLANES, stride=pairs), :] = value
        ones = jnp.ones((SUBLANES, flat.shape[1]), bf16)
        sums = []
        for r in range(SUBLANES):
            block = flat[r * pairs : (r + 1) * pairs, :].astype(bf16)
            payload[group * SUBLANES + r, :pairs, :] = block
            total = lax.dot_general(ones, block, (((1,), (1,)), ((), ())), preferred_element_type=f32)
            sums.append(total[:1])
        totals[group] = jnp.concatenate(sums, 0)

    if groups == 1:
        one_group(0)
    else:
        pl.loop(0, groups)(one_group)
    sums = totals[...].reshape(groups * SUBLANES, pairs)
    main = sums.astype(bf16)
    both = jnp.concatenate([main, (sums - main.astype(f32)).astype(bf16)], 0)
    for r in range(groups * SUBLANES):
        payload[r, pairs:, :] = both


def interpolate(fields, bracket, fraction):
    variables, levels, rows, columns = fields.shape
    plev = bracket.shape[0]
    groups = rows // SUBLANES
    pairs = variables * plev
    assert rows % SUBLANES == 0 and levels % 2 == 0 and pairs == columns
    grouped = fields.reshape(variables, levels, groups, SUBLANES, columns).transpose(2, 0, 1, 3, 4)
    grouped = grouped.reshape(groups, variables, levels // 2, 2 * SUBLANES, columns)
    bracket = bracket.reshape(plev, groups, SUBLANES, columns).transpose(1, 0, 2, 3)
    fraction = fraction.reshape(plev, groups, SUBLANES, columns).transpose(1, 0, 2, 3)
    return pl.pallas_call(
        functools.partial(interpolate_kernel, levels=levels),
        out_shape=jax.ShapeDtypeStruct((rows, pairs + 2 * rows, columns), bf16),
        in_specs=[VMEM] * 3,
        out_specs=VMEM,
        scratch_shapes=[
            pltpu.VMEM((SUBLANES * pairs, columns), f32),
            pltpu.VMEM((groups, SUBLANES, pairs), f32),
        ],
        name="interpolate",
    )(grouped, bracket, fraction)


def lay_kernel(received, whole, sem):
    parts, _, columns = received.shape
    pairs = whole.shape[0]
    copies = [
        pltpu.make_async_copy(
            received.at[j, :pairs], whole.at[:, j * columns : (j + 1) * columns], sem.at[j]
        )
        for j in range(parts)
    ]
    for copy in copies:
        copy.start()
    for copy in copies:
        copy.wait()


def lay(received, pairs):
    parts, _, columns = received.shape
    return pl.pallas_call(
        lay_kernel,
        out_shape=jax.ShapeDtypeStruct((pairs, parts * columns), bf16),
        in_specs=[pl.BlockSpec(memory_space=pl.ANY)],
        out_specs=pl.BlockSpec(memory_space=pl.ANY),
        scratch_shapes=[pltpu.SemaphoreType.DMA((parts,))],
        compiler_params=pltpu.CompilerParams(vmem_limit_bytes=1 << 20),
        cost_estimate=pl.CostEstimate(
            flops=2 * pairs * parts * columns * 1024, bytes_accessed=4 * pairs * parts * columns, transcendentals=0
        ),
        name="lay",
    )(received)


def shards(fields, bracket, fraction):
    variables, _, rows, columns = fields.shape
    plev = bracket.shape[0]
    pairs = variables * plev
    lon_count, lat_count = lax.axis_size("lon"), lax.axis_size("lat")
    lon_place, lat_place = lax.axis_index("lon"), lax.axis_index("lat")
    assert rows == lon_count

    payload = interpolate(fields, bracket, fraction)
    received = lax.all_to_all(payload, "lon", split_axis=0, concat_axis=0, tiled=True)

    sums = jnp.sum(received[:, pairs:].astype(f32), 0)
    means = (sums[:rows] + sums[rows:]) / f32(lon_count * columns)
    first_place, last_place = lon_place == 0, lon_place == lon_count - 1

    near = lon_place < lon_count // 2
    edge = jnp.where(near, means[rows - 1], means[0])
    ends = [((b, 0), (b - 1, 1)) for b in range(1, lat_count)]
    ends += [((b, lon_count - 1), (b + 1, lon_count - 2)) for b in range(lat_count - 1)]
    place = lambda at: at[1] * lat_count + at[0]
    swaps = [(place(s), place(t)) for s, t in ends] + [(place(t), place(s)) for s, t in ends]
    beyond = lax.ppermute(edge, ("lon", "lat"), swaps)

    on_pressure = lay(received, pairs)

    own = lax.dynamic_index_in_dim(means, lon_place, 0, False)
    below = lax.dynamic_index_in_dim(means, jnp.maximum(lon_place - 1, 0), 0, False)
    above = lax.dynamic_index_in_dim(means, jnp.minimum(lon_place + 1, rows - 1), 0, False)
    below = jnp.where(first_place, beyond, below)
    above = jnp.where(last_place, beyond, above)
    first_row = first_place & (lat_place == 0)
    last_row = last_place & (lat_place == lat_count - 1)
    meridional = jnp.where(
        first_row, above - own, jnp.where(last_row, own - below, 0.5 * (above - below))
    )
    return (
        on_pressure.reshape(variables, plev, 1, lon_count * columns),
        own.reshape(variables, plev, 1),
        meridional.reshape(variables, plev, 1),
    )


def solution(mesh):
    return jax.shard_map(
        shards,
        mesh=mesh,
        in_specs=(P(None, None, "lat", "lon"), P(None, "lat", "lon"), P(None, "lat", "lon")),
        out_specs=(
            P(None, None, ("lat", "lon"), None),
            P(None, None, ("lat", "lon")),
            P(None, None, ("lat", "lon")),
        ),
        check_vma=False,
    )
```

```python
import functools

import jax
import jax.numpy as jnp
from jax import lax
from jax.experimental import pallas as pl
from jax.experimental.pallas import tpu as pltpu
from jax.sharding import PartitionSpec as P

WINDOW = 16
FAR = (6, 4, 2)
SUBLANES = 8
bf16, f32 = jnp.bfloat16, jnp.float32
VMEM = pl.BlockSpec(memory_space=pltpu.VMEM)


def interpolate_kernel(fields, bracket, fraction, *refs, levels, order):
    *messages, flat, totals = refs
    places = [(message, i) for message in messages for i in range(message.shape[0])]
    groups, variables = fields.shape[:2]
    plev = bracket.shape[1]
    pairs = variables * plev
    step = levels // plev

    def one_group(group):
        for p in range(plev):
            base = min(p * step, levels - WINDOW)
            offset = bracket[group, p] - base
            index = jnp.concatenate([(offset + 1) >> 1, offset >> 1], 0).astype(f32).astype(bf16)
            high = index >= bf16(4)
            index = jnp.where(high, index - bf16(4), index)
            mid = index >= bf16(2)
            index = jnp.where(mid, index - bf16(2), index)
            low = index >= bf16(1)
            is_odd = (offset & 1) == 1
            weight = fraction[group, p].astype(f32)
            weight = jnp.where(is_odd, -weight, weight)
            for v in range(variables):
                w = [fields[group, v, base // 2 + k] for k in range(WINDOW // 2)]
                w = [jnp.where(low, w[k + 1], w[k]) for k in (0, 2, 4, 6)]
                w = [jnp.where(mid, w[k + 1], w[k]) for k in (0, 2)]
                picked = jnp.where(high, w[1], w[0]).astype(f32)
                even, odd = picked[:SUBLANES], picked[SUBLANES:]
                value = jnp.where(is_odd, odd, even) + weight * (odd - even)
                flat[pl.ds(v * plev + p, SUBLANES, stride=pairs), :] = value
        ones = jnp.ones((SUBLANES, flat.shape[1]), bf16)
        for r in range(SUBLANES):
            row = r
            if order:
                row = jnp.bitwise_xor(lax.axis_index("lon"), order[r])
            start = row * pairs if order is None else pl.multiple_of(row * pairs, pairs)
            block = flat[pl.ds(start, pairs), :].astype(bf16)
            if groups == 1:
                message, i = places[r]
                message[i, :pairs, :] = block
            else:
                messages[0][group * SUBLANES + r, :pairs, :] = block
            total = lax.dot_general(ones, block, (((1,), (1,)), ((), ())), preferred_element_type=f32)
            totals[group, pl.ds(row, 1)] = total[:1]

    if groups == 1:
        one_group(0)
    else:
        pl.loop(0, groups)(one_group)
    sums = totals[...].reshape(groups * SUBLANES, pairs)
    main = sums.astype(bf16)
    both = jnp.concatenate([main, (sums - main.astype(f32)).astype(bf16)], 0)
    for message, i in places:
        message[i, pairs:, :] = both


def interpolate(fields, bracket, fraction, sizes, order):
    variables, levels, rows, columns = fields.shape
    plev = bracket.shape[0]
    groups = rows // SUBLANES
    pairs = variables * plev
    assert rows % SUBLANES == 0 and levels % 2 == 0 and pairs == columns
    grouped = fields.reshape(variables, levels, groups, SUBLANES, columns).transpose(2, 0, 1, 3, 4)
    grouped = grouped.reshape(groups, variables, levels // 2, 2 * SUBLANES, columns)
    bracket = bracket.reshape(plev, groups, SUBLANES, columns).transpose(1, 0, 2, 3)
    fraction = fraction.reshape(plev, groups, SUBLANES, columns).transpose(1, 0, 2, 3)
    return pl.pallas_call(
        functools.partial(interpolate_kernel, levels=levels, order=order),
        out_shape=[jax.ShapeDtypeStruct((n, pairs + 2 * rows, columns), bf16) for n in sizes],
        in_specs=[VMEM] * 3,
        out_specs=[VMEM] * len(sizes),
        scratch_shapes=[
            pltpu.VMEM((SUBLANES * pairs, columns), f32),
            pltpu.VMEM((groups, SUBLANES, pairs), f32),
        ],
        name="interpolate",
    )(grouped, bracket, fraction)


def lay_kernel(*refs, pairs, order):
    *blocks, whole, sem = refs
    columns = blocks[0].shape[-1]
    parts = [(block, i) for block in blocks for i in range(block.shape[0])]
    copies = []
    for j, (block, i) in enumerate(parts):
        source = j if order is None else jnp.bitwise_xor(lax.axis_index("lon"), order[j])
        start = pl.multiple_of(source * columns, columns)
        copies.append(
            pltpu.make_async_copy(block.at[i, :pairs], whole.at[:, pl.ds(start, columns)], sem.at[j])
        )
    for copy in copies:
        copy.start()
    for copy in copies:
        copy.wait()


def lay(blocks, pairs, order):
    parts = sum(block.shape[0] for block in blocks)
    columns = blocks[0].shape[-1]
    anywhere = pl.BlockSpec(memory_space=pl.ANY)
    return pl.pallas_call(
        functools.partial(lay_kernel, pairs=pairs, order=order),
        out_shape=jax.ShapeDtypeStruct((pairs, parts * columns), bf16),
        in_specs=[anywhere] * len(blocks),
        out_specs=anywhere,
        scratch_shapes=[pltpu.SemaphoreType.DMA((parts,))],
        compiler_params=pltpu.CompilerParams(vmem_limit_bytes=1 << 20),
        cost_estimate=pl.CostEstimate(
            flops=2 * pairs * parts * columns * 1024, bytes_accessed=4 * pairs * parts * columns, transcendentals=0
        ),
        name="lay",
    )(*blocks)


def swap(value, mask):
    return lax.ppermute(value, "lon", [(i, i ^ mask) for i in range(lax.axis_size("lon"))])


def exchange(fields, bracket, fraction):
    count = lax.axis_size("lon")
    if count != SUBLANES:
        (payload,) = interpolate(fields, bracket, fraction, [count], None)
        return [lax.all_to_all(payload, "lon", split_axis=0, concat_axis=0, tiled=True)], None
    far = FAR
    order = [0, 1] + [mask ^ core for mask in far for core in (0, 1)]
    mine, other, *messages = interpolate(fields, bracket, fraction, [1, 1] + [2] * len(far), order)
    received = [swap(message, mask) for message, mask in zip(messages, far)]
    blocks = [mine, swap(other, 1)]
    for pair in received:
        blocks += [pair[:1], swap(pair[1:], 1)]
    return blocks, order


def shards(fields, bracket, fraction):
    variables, _, rows, columns = fields.shape
    plev = bracket.shape[0]
    pairs = variables * plev
    lon_count, lat_count = lax.axis_size("lon"), lax.axis_size("lat")
    lon_place, lat_place = lax.axis_index("lon"), lax.axis_index("lat")
    assert rows == lon_count

    blocks, order = exchange(fields, bracket, fraction)

    sums = sum(jnp.sum(block[:, pairs:].astype(f32), 0) for block in blocks)
    means = (sums[:rows] + sums[rows:]) / f32(lon_count * columns)
    first_place, last_place = lon_place == 0, lon_place == lon_count - 1

    near = lon_place < lon_count // 2
    edge = jnp.where(near, means[rows - 1], means[0])
    ends = [((b, 0), (b - 1, 1)) for b in range(1, lat_count)]
    ends += [((b, lon_count - 1), (b + 1, lon_count - 2)) for b in range(lat_count - 1)]
    place = lambda at: at[1] * lat_count + at[0]
    swaps = [(place(s), place(t)) for s, t in ends] + [(place(t), place(s)) for s, t in ends]
    beyond = lax.ppermute(edge, ("lon", "lat"), swaps)

    on_pressure = lay(blocks, pairs, order)

    own = lax.dynamic_index_in_dim(means, lon_place, 0, False)
    below = lax.dynamic_index_in_dim(means, jnp.maximum(lon_place - 1, 0), 0, False)
    above = lax.dynamic_index_in_dim(means, jnp.minimum(lon_place + 1, rows - 1), 0, False)
    below = jnp.where(first_place, beyond, below)
    above = jnp.where(last_place, beyond, above)
    first_row = first_place & (lat_place == 0)
    last_row = last_place & (lat_place == lat_count - 1)
    meridional = jnp.where(
        first_row, above - own, jnp.where(last_row, own - below, 0.5 * (above - below))
    )
    return (
        on_pressure.reshape(variables, plev, 1, lon_count * columns),
        own.reshape(variables, plev, 1),
        meridional.reshape(variables, plev, 1),
    )


def solution(mesh):
    return jax.shard_map(
        shards,
        mesh=mesh,
        in_specs=(P(None, None, "lat", "lon"), P(None, "lat", "lon"), P(None, "lat", "lon")),
        out_specs=(
            P(None, None, ("lat", "lon"), None),
            P(None, None, ("lat", "lon")),
            P(None, None, ("lat", "lon")),
        ),
        check_vma=False,
    )
```

```python
import functools

import jax
import jax.numpy as jnp
from jax import lax
from jax.experimental import pallas as pl
from jax.experimental.pallas import tpu as pltpu
from jax.sharding import PartitionSpec as P

WINDOW = 16
PLAN = ((6,), (4,), 3, 2, 1)
SUBLANES = 8
bf16, f32 = jnp.bfloat16, jnp.float32
VMEM = pl.BlockSpec(memory_space=pltpu.VMEM)


def interpolate_kernel(fields, bracket, fraction, *refs, levels, order):
    *messages, flat, totals = refs
    places = [(message, i) for message in messages for i in range(message.shape[0])]
    groups, variables = fields.shape[:2]
    plev = bracket.shape[1]
    pairs = variables * plev
    step = levels // plev

    def one_group(group):
        for p in range(plev):
            base = min(p * step, levels - WINDOW)
            offset = bracket[group, p] - base
            index = jnp.concatenate([(offset + 1) >> 1, offset >> 1], 0).astype(f32).astype(bf16)
            high = index >= bf16(4)
            index = jnp.where(high, index - bf16(4), index)
            mid = index >= bf16(2)
            index = jnp.where(mid, index - bf16(2), index)
            low = index >= bf16(1)
            is_odd = (offset & 1) == 1
            weight = fraction[group, p].astype(f32)
            weight = jnp.where(is_odd, -weight, weight)
            for v in range(variables):
                w = [fields[group, v, base // 2 + k] for k in range(WINDOW // 2)]
                w = [jnp.where(low, w[k + 1], w[k]) for k in (0, 2, 4, 6)]
                w = [jnp.where(mid, w[k + 1], w[k]) for k in (0, 2)]
                picked = jnp.where(high, w[1], w[0]).astype(f32)
                even, odd = picked[:SUBLANES], picked[SUBLANES:]
                value = jnp.where(is_odd, odd, even) + weight * (odd - even)
                flat[pl.ds(v * plev + p, SUBLANES, stride=pairs), :] = value
        ones = jnp.ones((SUBLANES, flat.shape[1]), bf16)
        for r in range(SUBLANES):
            row = r
            if order:
                row = jnp.bitwise_xor(lax.axis_index("lon"), order[r])
            start = row * pairs if order is None else pl.multiple_of(row * pairs, pairs)
            block = flat[pl.ds(start, pairs), :].astype(bf16)
            if groups == 1:
                message, i = places[r]
                message[i, :pairs, :] = block
            else:
                messages[0][group * SUBLANES + r, :pairs, :] = block
            total = lax.dot_general(ones, block, (((1,), (1,)), ((), ())), preferred_element_type=f32)
            totals[group, pl.ds(row, 1)] = total[:1]

    if groups == 1:
        one_group(0)
    else:
        pl.loop(0, groups)(one_group)
    sums = totals[...].reshape(groups * SUBLANES, pairs)
    main = sums.astype(bf16)
    both = jnp.concatenate([main, (sums - main.astype(f32)).astype(bf16)], 0)
    for message, i in places:
        message[i, pairs:, :] = both


def interpolate(fields, bracket, fraction, sizes, order):
    variables, levels, rows, columns = fields.shape
    plev = bracket.shape[0]
    groups = rows // SUBLANES
    pairs = variables * plev
    assert rows % SUBLANES == 0 and levels % 2 == 0 and pairs == columns
    grouped = fields.reshape(variables, levels, groups, SUBLANES, columns).transpose(2, 0, 1, 3, 4)
    grouped = grouped.reshape(groups, variables, levels // 2, 2 * SUBLANES, columns)
    bracket = bracket.reshape(plev, groups, SUBLANES, columns).transpose(1, 0, 2, 3)
    fraction = fraction.reshape(plev, groups, SUBLANES, columns).transpose(1, 0, 2, 3)
    return pl.pallas_call(
        functools.partial(interpolate_kernel, levels=levels, order=order),
        out_shape=[jax.ShapeDtypeStruct((n, pairs + 2 * rows, columns), bf16) for n in sizes],
        in_specs=[VMEM] * 3,
        out_specs=[VMEM] * len(sizes),
        scratch_shapes=[
            pltpu.VMEM((SUBLANES * pairs, columns), f32),
            pltpu.VMEM((groups, SUBLANES, pairs), f32),
        ],
        name="interpolate",
    )(grouped, bracket, fraction)


def lay_kernel(*refs, pairs, order):
    *blocks, whole, sem = refs
    columns = blocks[0].shape[-1]
    parts = [(block, i) for block in blocks for i in range(block.shape[0])]
    copies = []
    for j, (block, i) in enumerate(parts):
        source = j if order is None else jnp.bitwise_xor(lax.axis_index("lon"), order[j])
        start = pl.multiple_of(source * columns, columns)
        copies.append(
            pltpu.make_async_copy(block.at[i, :pairs], whole.at[:, pl.ds(start, columns)], sem.at[j])
        )
    for copy in copies:
        copy.start()
    for copy in copies:
        copy.wait()


def lay(blocks, pairs, order):
    parts = sum(block.shape[0] for block in blocks)
    columns = blocks[0].shape[-1]
    anywhere = pl.BlockSpec(memory_space=pl.ANY)
    return pl.pallas_call(
        functools.partial(lay_kernel, pairs=pairs, order=order),
        out_shape=jax.ShapeDtypeStruct((pairs, parts * columns), bf16),
        in_specs=[anywhere] * len(blocks),
        out_specs=anywhere,
        scratch_shapes=[pltpu.SemaphoreType.DMA((parts,))],
        compiler_params=pltpu.CompilerParams(vmem_limit_bytes=1 << 20),
        cost_estimate=pl.CostEstimate(
            flops=2 * pairs * parts * columns * 1024, bytes_accessed=4 * pairs * parts * columns, transcendentals=0
        ),
        name="lay",
    )(*blocks)


def swap(value, mask):
    return lax.ppermute(value, "lon", [(i, i ^ mask) for i in range(lax.axis_size("lon"))])


def edge_swaps(lon_count, lat_count):
    pairs = [((b, 0), (b - 1, 1)) for b in range(1, lat_count)]
    pairs += [((b, lon_count - 1), (b + 1, lon_count - 2)) for b in range(lat_count - 1)]
    taken = {place for pair in pairs for place in pair}
    masks = [mask for mask in (1, 3, 5, 4) if mask < lon_count]
    masks += [mask for mask in range(1, lon_count) if mask not in masks]
    for b in range(lat_count):
        for j in range(lon_count):
            if (b, j) not in taken:
                other = next((b, j ^ mask) for mask in masks if (b, j ^ mask) not in taken)
                taken |= {(b, j), other}
                pairs.append(((b, j), other))
    flat = [(s[1] * lat_count + s[0], t[1] * lat_count + t[0]) for s, t in pairs]
    return flat + [(t, s) for s, t in flat]


def exchange(fields, bracket, fraction):
    count = lax.axis_size("lon")
    if count != SUBLANES:
        (payload,) = interpolate(fields, bracket, fraction, [count], None)
        return [lax.all_to_all(payload, "lon", split_axis=0, concat_axis=0, tiled=True)], None
    plan = PLAN
    order = [0]
    for masks in plan:
        order += [masks] if isinstance(masks, int) else [masks[0], masks[0] ^ 1]
    sizes = [1] + [1 if isinstance(m, int) else 2 for m in plan]
    mine, *messages = interpolate(fields, bracket, fraction, sizes, order)
    received = [swap(message, m if isinstance(m, int) else m[0]) for message, m in zip(messages, plan)]
    blocks = [mine]
    for block, m in zip(received, plan):
        blocks += [block] if isinstance(m, int) else [block[:1], swap(block[1:], 1)]
    return blocks, order


def shards(fields, bracket, fraction):
    variables, _, rows, columns = fields.shape
    plev = bracket.shape[0]
    pairs = variables * plev
    lon_count, lat_count = lax.axis_size("lon"), lax.axis_size("lat")
    lon_place, lat_place = lax.axis_index("lon"), lax.axis_index("lat")
    assert rows == lon_count

    blocks, order = exchange(fields, bracket, fraction)

    sums = sum(jnp.sum(block[:, pairs:].astype(f32), 0) for block in blocks)
    means = (sums[:rows] + sums[rows:]) / f32(lon_count * columns)
    first_place, last_place = lon_place == 0, lon_place == lon_count - 1

    edge = jnp.where(lon_place < lon_count // 2, means[rows - 1], means[0])
    beyond = lax.ppermute(edge, ("lon", "lat"), edge_swaps(lon_count, lat_count))

    on_pressure = lay(blocks, pairs, order)

    own = lax.dynamic_index_in_dim(means, lon_place, 0, False)
    below = lax.dynamic_index_in_dim(means, jnp.maximum(lon_place - 1, 0), 0, False)
    above = lax.dynamic_index_in_dim(means, jnp.minimum(lon_place + 1, rows - 1), 0, False)
    below = jnp.where(first_place, beyond, below)
    above = jnp.where(last_place, beyond, above)
    first_row = first_place & (lat_place == 0)
    last_row = last_place & (lat_place == lat_count - 1)
    meridional = jnp.where(
        first_row, above - own, jnp.where(last_row, own - below, 0.5 * (above - below))
    )
    return (
        on_pressure.reshape(variables, plev, 1, lon_count * columns),
        own.reshape(variables, plev, 1),
        meridional.reshape(variables, plev, 1),
    )


def solution(mesh):
    return jax.shard_map(
        shards,
        mesh=mesh,
        in_specs=(P(None, None, "lat", "lon"), P(None, "lat", "lon"), P(None, "lat", "lon")),
        out_specs=(
            P(None, None, ("lat", "lon"), None),
            P(None, None, ("lat", "lon")),
            P(None, None, ("lat", "lon")),
        ),
        check_vma=False,
    )
```

```python
import functools

import jax
import jax.numpy as jnp
from jax import lax
from jax.experimental import pallas as pl
from jax.experimental.pallas import tpu as pltpu
from jax.sharding import PartitionSpec as P

WINDOW = 16
PLAN = ((6,), (4,), 3, 2, 1)
SUBLANES = 8
CHUNKS = 8
LIMIT = 8 << 20
bf16, f32 = jnp.bfloat16, jnp.float32
VMEM = pl.BlockSpec(memory_space=pltpu.VMEM)


def interpolate_kernel(fields, bracket, fraction, *refs, levels, order):
    *messages, flat, totals, near_fields, near_bracket, near_fraction, sem = refs
    places = [(message, i) for message in messages for i in range(message.shape[0])]
    groups, variables = fields.shape[:2]
    plev = bracket.shape[1]
    pairs = variables * plev
    step = levels // plev
    chunks = max(n for n in range(1, CHUNKS + 1) if (levels // 2) % n == 0)
    depth = levels // 2 // chunks

    def one_group(group):
        copies = [
            pltpu.make_async_copy(bracket.at[group], near_bracket.at[0], sem.at[chunks]),
            pltpu.make_async_copy(fraction.at[group], near_fraction.at[0], sem.at[chunks + 1]),
        ]
        copies += [
            pltpu.make_async_copy(
                fields.at[group, :, pl.ds(n * depth, depth)],
                near_fields.at[0, :, pl.ds(n * depth, depth)],
                sem.at[n],
            )
            for n in range(chunks)
        ]
        for copy in copies:
            copy.start()
        copies[0].wait()
        copies[1].wait()
        interpolate_group(group, copies[2:])

    def interpolate_group(group, arriving):
        for p in range(plev):
            base = min(p * step, levels - WINDOW)
            while arriving and (base + WINDOW) // 2 > depth * (chunks - len(arriving)):
                arriving.pop(0).wait()
            offset = near_bracket[0, p] - base
            index = jnp.concatenate([(offset + 1) >> 1, offset >> 1], 0).astype(f32).astype(bf16)
            high = index >= bf16(4)
            index = jnp.where(high, index - bf16(4), index)
            mid = index >= bf16(2)
            index = jnp.where(mid, index - bf16(2), index)
            low = index >= bf16(1)
            is_odd = (offset & 1) == 1
            weight = near_fraction[0, p].astype(f32)
            weight = jnp.where(is_odd, -weight, weight)
            for v in range(variables):
                w = [near_fields[0, v, base // 2 + k] for k in range(WINDOW // 2)]
                w = [jnp.where(low, w[k + 1], w[k]) for k in (0, 2, 4, 6)]
                w = [jnp.where(mid, w[k + 1], w[k]) for k in (0, 2)]
                picked = jnp.where(high, w[1], w[0]).astype(f32)
                even, odd = picked[:SUBLANES], picked[SUBLANES:]
                value = jnp.where(is_odd, odd, even) + weight * (odd - even)
                flat[pl.ds(v * plev + p, SUBLANES, stride=pairs), :] = value
        ones = jnp.ones((SUBLANES, flat.shape[1]), bf16)
        for r in range(SUBLANES):
            row = r
            if order:
                row = jnp.bitwise_xor(lax.axis_index("lon"), order[r])
            start = row * pairs if order is None else pl.multiple_of(row * pairs, pairs)
            block = flat[pl.ds(start, pairs), :].astype(bf16)
            if groups == 1:
                message, i = places[r]
                message[i, :pairs, :] = block
            else:
                messages[0][group * SUBLANES + r, :pairs, :] = block
            total = lax.dot_general(ones, block, (((1,), (1,)), ((), ())), preferred_element_type=f32)
            totals[group, pl.ds(row, 1)] = total[:1]

    if groups == 1:
        one_group(0)
    else:
        pl.loop(0, groups)(one_group)
    sums = totals[...].reshape(groups * SUBLANES, pairs)
    main = sums.astype(bf16)
    both = jnp.concatenate([main, (sums - main.astype(f32)).astype(bf16)], 0)
    for message, i in places:
        message[i, pairs:, :] = both


def interpolate(fields, bracket, fraction, sizes, order):
    variables, levels, rows, columns = fields.shape
    plev = bracket.shape[0]
    groups = rows // SUBLANES
    pairs = variables * plev
    assert rows % SUBLANES == 0 and levels % 2 == 0 and pairs == columns
    grouped = fields.reshape(variables, levels, groups, SUBLANES, columns).transpose(2, 0, 1, 3, 4)
    grouped = grouped.reshape(groups, variables, levels // 2, 2 * SUBLANES, columns)
    bracket = bracket.reshape(plev, groups, SUBLANES, columns).transpose(1, 0, 2, 3)
    fraction = fraction.reshape(plev, groups, SUBLANES, columns).transpose(1, 0, 2, 3)
    return pl.pallas_call(
        functools.partial(interpolate_kernel, levels=levels, order=order),
        out_shape=[jax.ShapeDtypeStruct((n, pairs + 2 * rows, columns), bf16) for n in sizes],
        in_specs=[pl.BlockSpec(memory_space=pltpu.HBM)] * 3,
        out_specs=[VMEM] * len(sizes),
        scratch_shapes=[
            pltpu.VMEM((SUBLANES * pairs, columns), f32),
            pltpu.VMEM((groups, SUBLANES, pairs), f32),
            pltpu.VMEM((1,) + grouped.shape[1:], bf16),
            pltpu.VMEM((1,) + bracket.shape[1:], jnp.int32),
            pltpu.VMEM((1,) + fraction.shape[1:], bf16),
            pltpu.SemaphoreType.DMA((CHUNKS + 2,)),
        ],
        compiler_params=pltpu.CompilerParams(vmem_limit_bytes=LIMIT),
        name="interpolate",
    )(*(pltpu.with_memory_space_constraint(x, pltpu.HBM) for x in (grouped, bracket, fraction)))


def lay_kernel(*refs, pairs, order):
    *blocks, whole, sem = refs
    columns = blocks[0].shape[-1]
    parts = [(block, i) for block in blocks for i in range(block.shape[0])]
    copies = []
    for j, (block, i) in enumerate(parts):
        source = j if order is None else jnp.bitwise_xor(lax.axis_index("lon"), order[j])
        start = pl.multiple_of(source * columns, columns)
        copies.append(
            pltpu.make_async_copy(block.at[i, :pairs], whole.at[:, pl.ds(start, columns)], sem.at[j])
        )
    for copy in copies:
        copy.start()
    for copy in copies:
        copy.wait()


def lay(blocks, pairs, order):
    parts = sum(block.shape[0] for block in blocks)
    columns = blocks[0].shape[-1]
    anywhere = pl.BlockSpec(memory_space=pl.ANY)
    return pl.pallas_call(
        functools.partial(lay_kernel, pairs=pairs, order=order),
        out_shape=jax.ShapeDtypeStruct((pairs, parts * columns), bf16),
        in_specs=[anywhere] * len(blocks),
        out_specs=anywhere,
        scratch_shapes=[pltpu.SemaphoreType.DMA((parts,))],
        compiler_params=pltpu.CompilerParams(vmem_limit_bytes=1 << 20),
        cost_estimate=pl.CostEstimate(
            flops=2 * pairs * parts * columns * 1024, bytes_accessed=4 * pairs * parts * columns, transcendentals=0
        ),
        name="lay",
    )(*blocks)


def swap(value, mask):
    return lax.ppermute(value, "lon", [(i, i ^ mask) for i in range(lax.axis_size("lon"))])


def edge_swaps(lon_count, lat_count):
    pairs = [((b, 0), (b - 1, 1)) for b in range(1, lat_count)]
    pairs += [((b, lon_count - 1), (b + 1, lon_count - 2)) for b in range(lat_count - 1)]
    taken = {place for pair in pairs for place in pair}
    masks = [mask for mask in (1, 3, 5, 4) if mask < lon_count]
    masks += [mask for mask in range(1, lon_count) if mask not in masks]
    for b in range(lat_count):
        for j in range(lon_count):
            if (b, j) not in taken:
                other = next((b, j ^ mask) for mask in masks if (b, j ^ mask) not in taken)
                taken |= {(b, j), other}
                pairs.append(((b, j), other))
    flat = [(s[1] * lat_count + s[0], t[1] * lat_count + t[0]) for s, t in pairs]
    return flat + [(t, s) for s, t in flat]


def exchange(fields, bracket, fraction):
    count = lax.axis_size("lon")
    if count != SUBLANES:
        (payload,) = interpolate(fields, bracket, fraction, [count], None)
        return [lax.all_to_all(payload, "lon", split_axis=0, concat_axis=0, tiled=True)], None
    plan = PLAN
    order = [0]
    for masks in plan:
        order += [masks] if isinstance(masks, int) else [masks[0], masks[0] ^ 1]
    sizes = [1] + [1 if isinstance(m, int) else 2 for m in plan]
    mine, *messages = interpolate(fields, bracket, fraction, sizes, order)
    received = [swap(message, m if isinstance(m, int) else m[0]) for message, m in zip(messages, plan)]
    blocks = [mine]
    for block, m in zip(received, plan):
        blocks += [block] if isinstance(m, int) else [block[:1], swap(block[1:], 1)]
    return blocks, order


def shards(fields, bracket, fraction):
    variables, _, rows, columns = fields.shape
    plev = bracket.shape[0]
    pairs = variables * plev
    lon_count, lat_count = lax.axis_size("lon"), lax.axis_size("lat")
    lon_place, lat_place = lax.axis_index("lon"), lax.axis_index("lat")
    assert rows == lon_count

    blocks, order = exchange(fields, bracket, fraction)

    sums = sum(jnp.sum(block[:, pairs:].astype(f32), 0) for block in blocks)
    means = (sums[:rows] + sums[rows:]) / f32(lon_count * columns)
    first_place, last_place = lon_place == 0, lon_place == lon_count - 1

    edge = jnp.where(lon_place < lon_count // 2, means[rows - 1], means[0])
    beyond = lax.ppermute(edge, ("lon", "lat"), edge_swaps(lon_count, lat_count))

    on_pressure = lay(blocks, pairs, order)

    own = lax.dynamic_index_in_dim(means, lon_place, 0, False)
    below = lax.dynamic_index_in_dim(means, jnp.maximum(lon_place - 1, 0), 0, False)
    above = lax.dynamic_index_in_dim(means, jnp.minimum(lon_place + 1, rows - 1), 0, False)
    below = jnp.where(first_place, beyond, below)
    above = jnp.where(last_place, beyond, above)
    first_row = first_place & (lat_place == 0)
    last_row = last_place & (lat_place == lat_count - 1)
    meridional = jnp.where(
        first_row, above - own, jnp.where(last_row, own - below, 0.5 * (above - below))
    )
    return (
        on_pressure.reshape(variables, plev, 1, lon_count * columns),
        own.reshape(variables, plev, 1),
        meridional.reshape(variables, plev, 1),
    )


def solution(mesh):
    return jax.shard_map(
        shards,
        mesh=mesh,
        in_specs=(P(None, None, "lat", "lon"), P(None, "lat", "lon"), P(None, "lat", "lon")),
        out_specs=(
            P(None, None, ("lat", "lon"), None),
            P(None, None, ("lat", "lon")),
            P(None, None, ("lat", "lon")),
        ),
        check_vma=False,
    )
```

```python
import functools

import jax
import jax.numpy as jnp
from jax import lax
from jax.experimental import pallas as pl
from jax.experimental.pallas import tpu as pltpu
from jax.sharding import PartitionSpec as P

WINDOW = 16
PLAN = ((5,), (7,), 3, 2, 1)
SUBLANES = 8
CHUNKS = 4
PAD = 8
LIMIT = 8 << 20
bf16, f32 = jnp.bfloat16, jnp.float32
VMEM = pl.BlockSpec(memory_space=pltpu.VMEM)


def interpolate_kernel(fields, bracket, fraction, *refs, levels, order):
    *messages, flat, totals, near_fields, near_bracket, near_fraction, sem = refs
    places = [(message, i) for message in messages for i in range(message.shape[0])]
    groups, variables = fields.shape[:2]
    plev = bracket.shape[1]
    pairs = variables * plev
    step = levels // plev
    chunks = max(n for n in range(1, CHUNKS + 1) if (levels // 2) % n == 0)
    depth = levels // 2 // chunks

    def one_group(group):
        copies = [
            pltpu.make_async_copy(bracket.at[group], near_bracket.at[0], sem.at[chunks]),
            pltpu.make_async_copy(fraction.at[group], near_fraction.at[0], sem.at[chunks + 1]),
        ]
        copies += [
            pltpu.make_async_copy(
                fields.at[group, :, pl.ds(n * depth, depth)],
                near_fields.at[0, :, pl.ds(n * depth, depth)],
                sem.at[n],
            )
            for n in range(chunks)
        ]
        for copy in copies:
            copy.start()
        copies[0].wait()
        copies[1].wait()
        interpolate_group(group, copies[2:])

    def interpolate_group(group, arriving):
        for p in range(plev):
            base = min(p * step, levels - WINDOW)
            while arriving and (base + WINDOW) // 2 > depth * (chunks - len(arriving)):
                arriving.pop(0).wait()
            offset = near_bracket[0, p] - base
            index = jnp.concatenate([(offset + 1) >> 1, offset >> 1], 0).astype(f32).astype(bf16)
            high = index >= bf16(4)
            index = jnp.where(high, index - bf16(4), index)
            mid = index >= bf16(2)
            index = jnp.where(mid, index - bf16(2), index)
            low = index >= bf16(1)
            is_odd = (offset & 1) == 1
            weight = near_fraction[0, p].astype(f32)
            weight = jnp.where(is_odd, -weight, weight)
            for v in range(variables):
                w = [near_fields[0, v, base // 2 + k] for k in range(WINDOW // 2)]
                w = [jnp.where(low, w[k + 1], w[k]) for k in (0, 2, 4, 6)]
                w = [jnp.where(mid, w[k + 1], w[k]) for k in (0, 2)]
                picked = jnp.where(high, w[1], w[0]).astype(f32)
                even, odd = picked[:SUBLANES], picked[SUBLANES:]
                value = jnp.where(is_odd, odd, even) + weight * (odd - even)
                flat[pl.ds(v * plev + p, SUBLANES, stride=pairs + PAD), :] = value
        ones = jnp.ones((SUBLANES, flat.shape[1]), bf16)
        for r in range(SUBLANES):
            row = r
            if order:
                row = jnp.bitwise_xor(lax.axis_index("lon"), order[r])
            start = row * (pairs + PAD) if order is None else pl.multiple_of(row * (pairs + PAD), 8)
            block = flat[pl.ds(start, pairs), :].astype(bf16)
            if groups == 1:
                message, i = places[r]
                message[i, :pairs, :] = block
            else:
                messages[0][group * SUBLANES + r, :pairs, :] = block
            total = lax.dot_general(ones, block, (((1,), (1,)), ((), ())), preferred_element_type=f32)
            totals[group, pl.ds(row, 1)] = total[:1]

    if groups == 1:
        one_group(0)
    else:
        pl.loop(0, groups)(one_group)
    sums = totals[...].reshape(groups * SUBLANES, pairs)
    main = sums.astype(bf16)
    both = jnp.concatenate([main, (sums - main.astype(f32)).astype(bf16)], 0)
    for message, i in places:
        message[i, pairs:, :] = both


def interpolate(fields, bracket, fraction, sizes, order):
    variables, levels, rows, columns = fields.shape
    plev = bracket.shape[0]
    groups = rows // SUBLANES
    pairs = variables * plev
    assert rows % SUBLANES == 0 and levels % 2 == 0 and pairs == columns
    grouped = fields.reshape(variables, levels, groups, SUBLANES, columns).transpose(2, 0, 1, 3, 4)
    grouped = grouped.reshape(groups, variables, levels // 2, 2 * SUBLANES, columns)
    bracket = bracket.reshape(plev, groups, SUBLANES, columns).transpose(1, 0, 2, 3)
    fraction = fraction.reshape(plev, groups, SUBLANES, columns).transpose(1, 0, 2, 3)
    return pl.pallas_call(
        functools.partial(interpolate_kernel, levels=levels, order=order),
        out_shape=[jax.ShapeDtypeStruct((n, pairs + 2 * rows, columns), bf16) for n in sizes],
        in_specs=[pl.BlockSpec(memory_space=pltpu.HBM)] * 3,
        out_specs=[VMEM] * len(sizes),
        scratch_shapes=[
            pltpu.VMEM((SUBLANES * (pairs + PAD), columns), f32),
            pltpu.VMEM((groups, SUBLANES, pairs), f32),
            pltpu.VMEM((1,) + grouped.shape[1:], bf16),
            pltpu.VMEM((1,) + bracket.shape[1:], jnp.int32),
            pltpu.VMEM((1,) + fraction.shape[1:], bf16),
            pltpu.SemaphoreType.DMA((CHUNKS + 2,)),
        ],
        compiler_params=pltpu.CompilerParams(vmem_limit_bytes=LIMIT),
        name="interpolate",
    )(*(pltpu.with_memory_space_constraint(x, pltpu.HBM) for x in (grouped, bracket, fraction)))


def lay_kernel(*refs, pairs, order):
    *blocks, whole, sem = refs
    columns = blocks[0].shape[-1]
    parts = [(block, i) for block in blocks for i in range(block.shape[0])]
    copies = []
    for j, (block, i) in enumerate(parts):
        source = j if order is None else jnp.bitwise_xor(lax.axis_index("lon"), order[j])
        start = pl.multiple_of(source * columns, columns)
        copies.append(
            pltpu.make_async_copy(block.at[i, :pairs], whole.at[:, pl.ds(start, columns)], sem.at[j])
        )
    for copy in copies:
        copy.start()
    for copy in copies:
        copy.wait()


def lay(blocks, pairs, order):
    parts = sum(block.shape[0] for block in blocks)
    columns = blocks[0].shape[-1]
    anywhere = pl.BlockSpec(memory_space=pl.ANY)
    return pl.pallas_call(
        functools.partial(lay_kernel, pairs=pairs, order=order),
        out_shape=jax.ShapeDtypeStruct((pairs, parts * columns), bf16),
        in_specs=[anywhere] * len(blocks),
        out_specs=anywhere,
        scratch_shapes=[pltpu.SemaphoreType.DMA((parts,))],
        compiler_params=pltpu.CompilerParams(vmem_limit_bytes=1 << 20),
        cost_estimate=pl.CostEstimate(
            flops=2 * pairs * parts * columns * 1024, bytes_accessed=4 * pairs * parts * columns, transcendentals=0
        ),
        name="lay",
    )(*blocks)


def swap(value, mask):
    return lax.ppermute(value, "lon", [(i, i ^ mask) for i in range(lax.axis_size("lon"))])


def edge_swaps(lon_count, lat_count):
    pairs = [((b, 0), (b - 1, 1)) for b in range(1, lat_count)]
    pairs += [((b, lon_count - 1), (b + 1, lon_count - 2)) for b in range(lat_count - 1)]
    taken = {place for pair in pairs for place in pair}
    masks = [mask for mask in (1, 3, 5, 4) if mask < lon_count]
    masks += [mask for mask in range(1, lon_count) if mask not in masks]
    for b in range(lat_count):
        for j in range(lon_count):
            if (b, j) not in taken:
                other = next((b, j ^ mask) for mask in masks if (b, j ^ mask) not in taken)
                taken |= {(b, j), other}
                pairs.append(((b, j), other))
    flat = [(s[1] * lat_count + s[0], t[1] * lat_count + t[0]) for s, t in pairs]
    return flat + [(t, s) for s, t in flat]


def exchange(fields, bracket, fraction):
    count = lax.axis_size("lon")
    if count != SUBLANES:
        (payload,) = interpolate(fields, bracket, fraction, [count], None)
        return [lax.all_to_all(payload, "lon", split_axis=0, concat_axis=0, tiled=True)], None
    plan = PLAN
    order = [0]
    for masks in plan:
        order += [masks] if isinstance(masks, int) else [masks[0], masks[0] ^ 1]
    sizes = [1] + [1 if isinstance(m, int) else 2 for m in plan]
    mine, *messages = interpolate(fields, bracket, fraction, sizes, order)
    received = [swap(message, m if isinstance(m, int) else m[0]) for message, m in zip(messages, plan)]
    blocks = [mine]
    for block, m in zip(received, plan):
        blocks += [block] if isinstance(m, int) else [block[:1], swap(block[1:], 1)]
    return blocks, order


def shards(fields, bracket, fraction):
    variables, _, rows, columns = fields.shape
    plev = bracket.shape[0]
    pairs = variables * plev
    lon_count, lat_count = lax.axis_size("lon"), lax.axis_size("lat")
    lon_place, lat_place = lax.axis_index("lon"), lax.axis_index("lat")
    assert rows == lon_count

    blocks, order = exchange(fields, bracket, fraction)

    sums = sum(jnp.sum(block[:, pairs:].astype(f32), 0) for block in blocks)
    means = (sums[:rows] + sums[rows:]) / f32(lon_count * columns)
    first_place, last_place = lon_place == 0, lon_place == lon_count - 1

    edge = jnp.where(lon_place < lon_count // 2, means[rows - 1], means[0])
    beyond = lax.ppermute(edge, ("lon", "lat"), edge_swaps(lon_count, lat_count))

    on_pressure = lay(blocks, pairs, order)

    own = lax.dynamic_index_in_dim(means, lon_place, 0, False)
    below = lax.dynamic_index_in_dim(means, jnp.maximum(lon_place - 1, 0), 0, False)
    above = lax.dynamic_index_in_dim(means, jnp.minimum(lon_place + 1, rows - 1), 0, False)
    below = jnp.where(first_place, beyond, below)
    above = jnp.where(last_place, beyond, above)
    first_row = first_place & (lat_place == 0)
    last_row = last_place & (lat_place == lat_count - 1)
    meridional = jnp.where(
        first_row, above - own, jnp.where(last_row, own - below, 0.5 * (above - below))
    )
    return (
        on_pressure.reshape(variables, plev, 1, lon_count * columns),
        own.reshape(variables, plev, 1),
        meridional.reshape(variables, plev, 1),
    )


def solution(mesh):
    return jax.shard_map(
        shards,
        mesh=mesh,
        in_specs=(P(None, None, "lat", "lon"), P(None, "lat", "lon"), P(None, "lat", "lon")),
        out_specs=(
            P(None, None, ("lat", "lon"), None),
            P(None, None, ("lat", "lon")),
            P(None, None, ("lat", "lon")),
        ),
        check_vma=False,
    )
```

```python
import functools

import jax
import jax.numpy as jnp
from jax import lax
from jax.experimental import pallas as pl
from jax.experimental.pallas import tpu as pltpu
from jax.sharding import PartitionSpec as P

WINDOW = 16
PLAN = ((5,), (7,), 3, 2, 1)
SUBLANES = 8
CHUNKS = 4
PAD = 8
LIMIT = 8 << 20
bf16, f32 = jnp.bfloat16, jnp.float32
VMEM = pl.BlockSpec(memory_space=pltpu.VMEM)


def interpolate_kernel(fields, bracket, fraction, *refs, levels, order):
    *messages, flat, totals, near_fields, near_bracket, near_fraction, sem = refs
    places = [(message, i) for message in messages for i in range(message.shape[0])]
    groups, variables = fields.shape[:2]
    plev = bracket.shape[1]
    pairs = variables * plev
    step = levels // plev
    chunks = max(n for n in range(1, CHUNKS + 1) if (levels // 2) % n == 0)
    depth = levels // 2 // chunks

    def one_group(group):
        copies = [
            pltpu.make_async_copy(bracket.at[group], near_bracket.at[0], sem.at[chunks]),
            pltpu.make_async_copy(fraction.at[group], near_fraction.at[0], sem.at[chunks + 1]),
        ]
        copies += [
            pltpu.make_async_copy(
                fields.at[group, :, pl.ds(n * depth, depth)],
                near_fields.at[0, :, pl.ds(n * depth, depth)],
                sem.at[n],
            )
            for n in range(chunks)
        ]
        for copy in copies:
            copy.start()
        copies[0].wait()
        copies[1].wait()
        interpolate_group(group, copies[2:])

    def interpolate_group(group, arriving):
        for p in range(plev):
            base = min(p * step, levels - WINDOW)
            while arriving and (base + WINDOW) // 2 > depth * (chunks - len(arriving)):
                arriving.pop(0).wait()
            offset = near_bracket[0, p] - base
            index = jnp.concatenate([(offset + 1) >> 1, offset >> 1], 0).astype(f32).astype(bf16)
            high = index >= bf16(4)
            index = jnp.where(high, index - bf16(4), index)
            mid = index >= bf16(2)
            index = jnp.where(mid, index - bf16(2), index)
            low = index >= bf16(1)
            is_odd = (offset & 1) == 1
            weight = near_fraction[0, p].astype(f32)
            weight = jnp.where(is_odd, -weight, weight)
            for v in range(variables):
                w = [near_fields[0, v, base // 2 + k] for k in range(WINDOW // 2)]
                w = [jnp.where(low, w[k + 1], w[k]) for k in (0, 2, 4, 6)]
                w = [jnp.where(mid, w[k + 1], w[k]) for k in (0, 2)]
                picked = jnp.where(high, w[1], w[0]).astype(f32)
                even, odd = picked[:SUBLANES], picked[SUBLANES:]
                value = jnp.where(is_odd, odd, even) + weight * (odd - even)
                flat[pl.ds(v * plev + p, SUBLANES, stride=pairs + PAD), :] = value
        ones = jnp.ones((SUBLANES, flat.shape[1]), bf16)
        for r in range(SUBLANES):
            row = r
            if order:
                row = jnp.bitwise_xor(lax.axis_index("lon"), order[r])
            start = row * (pairs + PAD) if order is None else pl.multiple_of(row * (pairs + PAD), 8)
            block = flat[pl.ds(start, pairs), :].astype(bf16)
            if groups == 1:
                message, i = places[r]
                message[i, :pairs, :] = block
            else:
                messages[0][group * SUBLANES + r, :pairs, :] = block
            total = lax.dot_general(ones, block, (((1,), (1,)), ((), ())), preferred_element_type=f32)
            totals[group, pl.ds(row, 1)] = total[:1]

    if groups == 1:
        one_group(0)
    else:
        pl.loop(0, groups)(one_group)
    sums = totals[...].reshape(groups * SUBLANES, pairs)
    main = sums.astype(bf16)
    both = jnp.concatenate([main, (sums - main.astype(f32)).astype(bf16)], 0)
    for message, i in places:
        message[i, pairs:, :] = both


def interpolate(fields, bracket, fraction, sizes, order):
    variables, levels, rows, columns = fields.shape
    plev = bracket.shape[0]
    groups = rows // SUBLANES
    pairs = variables * plev
    assert rows % SUBLANES == 0 and levels % 2 == 0 and pairs == columns
    grouped = fields.reshape(variables, levels, groups, SUBLANES, columns).transpose(2, 0, 1, 3, 4)
    grouped = grouped.reshape(groups, variables, levels // 2, 2 * SUBLANES, columns)
    bracket = bracket.reshape(plev, groups, SUBLANES, columns).transpose(1, 0, 2, 3)
    fraction = fraction.reshape(plev, groups, SUBLANES, columns).transpose(1, 0, 2, 3)
    return pl.pallas_call(
        functools.partial(interpolate_kernel, levels=levels, order=order),
        out_shape=[jax.ShapeDtypeStruct((n, pairs + 2 * rows, columns), bf16) for n in sizes],
        in_specs=[pl.BlockSpec(memory_space=pltpu.HBM)] * 3,
        out_specs=[VMEM] * len(sizes),
        scratch_shapes=[
            pltpu.VMEM((SUBLANES * (pairs + PAD), columns), f32),
            pltpu.VMEM((groups, SUBLANES, pairs), f32),
            pltpu.VMEM((1,) + grouped.shape[1:], bf16),
            pltpu.VMEM((1,) + bracket.shape[1:], jnp.int32),
            pltpu.VMEM((1,) + fraction.shape[1:], bf16),
            pltpu.SemaphoreType.DMA((CHUNKS + 2,)),
        ],
        compiler_params=pltpu.CompilerParams(vmem_limit_bytes=LIMIT),
        name="interpolate",
    )(*(pltpu.with_memory_space_constraint(x, pltpu.HBM) for x in (grouped, bracket, fraction)))


def lay_kernel(*refs, pairs, order):
    *blocks, whole, sem = refs
    columns = blocks[0].shape[-1]
    parts = [(block, i) for block in blocks for i in range(block.shape[0])]
    copies = []
    for j, (block, i) in enumerate(parts):
        source = j if order is None else jnp.bitwise_xor(lax.axis_index("lon"), order[j])
        start = pl.multiple_of(source * columns, columns)
        copies.append(
            pltpu.make_async_copy(block.at[i, :pairs], whole.at[:, pl.ds(start, columns)], sem.at[j])
        )
    for copy in copies:
        copy.start()
    for copy in copies:
        copy.wait()


def lay(blocks, pairs, order):
    parts = sum(block.shape[0] for block in blocks)
    columns = blocks[0].shape[-1]
    anywhere = pl.BlockSpec(memory_space=pl.ANY)
    return pl.pallas_call(
        functools.partial(lay_kernel, pairs=pairs, order=order),
        out_shape=jax.ShapeDtypeStruct((pairs, parts * columns), bf16),
        in_specs=[anywhere] * len(blocks),
        out_specs=anywhere,
        scratch_shapes=[pltpu.SemaphoreType.DMA((parts,))],
        compiler_params=pltpu.CompilerParams(vmem_limit_bytes=1 << 20),
        cost_estimate=pl.CostEstimate(
            flops=2 * pairs * parts * columns * 1024, bytes_accessed=4 * pairs * parts * columns, transcendentals=0
        ),
        name="lay",
    )(*blocks)


def swap(value, mask):
    return lax.ppermute(value, "lon", [(i, i ^ mask) for i in range(lax.axis_size("lon"))])


def edge_routes(lon_count, lat_count):
    routes = []
    start = 1
    if lon_count == 8 and lat_count > 1:
        ring = [(0, 3), (1, 0), (1, 2), (1, 3), (0, 2), (0, 6)]
        routes += list(zip(ring, ring[1:] + ring[:1]))
        start = 2
    pairs = [((b, 0), (b - 1, 1)) for b in range(start, lat_count)]
    pairs += [((b, lon_count - 1), (b + 1, lon_count - 2)) for b in range(lat_count - 1)]
    taken = {place for pair in pairs + routes for place in pair}
    masks = [mask for mask in (1, 3, 5, 4) if mask < lon_count]
    masks += [mask for mask in range(1, lon_count) if mask not in masks]
    for b in range(lat_count):
        for j in range(lon_count):
            if (b, j) not in taken:
                other = next((b, j ^ mask) for mask in masks if (b, j ^ mask) not in taken)
                taken |= {(b, j), other}
                pairs.append(((b, j), other))
    routes += pairs + [(t, s) for s, t in pairs]
    return [(s[1] * lat_count + s[0], t[1] * lat_count + t[0]) for s, t in routes]


def exchange(fields, bracket, fraction):
    count = lax.axis_size("lon")
    if count != SUBLANES:
        (payload,) = interpolate(fields, bracket, fraction, [count], None)
        return [lax.all_to_all(payload, "lon", split_axis=0, concat_axis=0, tiled=True)], None
    plan = PLAN
    order = [0]
    for masks in plan:
        order += [masks] if isinstance(masks, int) else [masks[0], masks[0] ^ 1]
    sizes = [1] + [1 if isinstance(m, int) else 2 for m in plan]
    mine, *messages = interpolate(fields, bracket, fraction, sizes, order)
    received = [swap(message, m if isinstance(m, int) else m[0]) for message, m in zip(messages, plan)]
    blocks = [mine]
    for block, m in zip(received, plan):
        blocks += [block] if isinstance(m, int) else [block[:1], swap(block[1:], 1)]
    return blocks, order


def shards(fields, bracket, fraction):
    variables, _, rows, columns = fields.shape
    plev = bracket.shape[0]
    pairs = variables * plev
    lon_count, lat_count = lax.axis_size("lon"), lax.axis_size("lat")
    lon_place, lat_place = lax.axis_index("lon"), lax.axis_index("lat")
    assert rows == lon_count

    blocks, order = exchange(fields, bracket, fraction)

    sums = sum(jnp.sum(block[:, pairs:].astype(f32), 0) for block in blocks)
    means = (sums[:rows] + sums[rows:]) / f32(lon_count * columns)
    first_place, last_place = lon_place == 0, lon_place == lon_count - 1

    edge = jnp.where(lon_place < lon_count // 2, means[rows - 1], means[0])
    beyond = lax.ppermute(edge, ("lon", "lat"), edge_routes(lon_count, lat_count))

    on_pressure = lay(blocks, pairs, order)

    own = lax.dynamic_index_in_dim(means, lon_place, 0, False)
    below = lax.dynamic_index_in_dim(means, jnp.maximum(lon_place - 1, 0), 0, False)
    above = lax.dynamic_index_in_dim(means, jnp.minimum(lon_place + 1, rows - 1), 0, False)
    below = jnp.where(first_place, beyond, below)
    above = jnp.where(last_place, beyond, above)
    first_row = first_place & (lat_place == 0)
    last_row = last_place & (lat_place == lat_count - 1)
    meridional = jnp.where(
        first_row, above - own, jnp.where(last_row, own - below, 0.5 * (above - below))
    )
    return (
        on_pressure.reshape(variables, plev, 1, lon_count * columns),
        own.reshape(variables, plev, 1),
        meridional.reshape(variables, plev, 1),
    )


def solution(mesh):
    return jax.shard_map(
        shards,
        mesh=mesh,
        in_specs=(P(None, None, "lat", "lon"), P(None, "lat", "lon"), P(None, "lat", "lon")),
        out_specs=(
            P(None, None, ("lat", "lon"), None),
            P(None, None, ("lat", "lon")),
            P(None, None, ("lat", "lon")),
        ),
        check_vma=False,
    )
```

```python
import functools

import jax
import jax.numpy as jnp
from jax import lax
from jax.experimental import pallas as pl
from jax.experimental.pallas import tpu as pltpu
from jax.sharding import PartitionSpec as P

WINDOW = 16
AFTER = (7,)
BEFORE = (3, 5)
SUBLANES = 8
CHUNKS = 4
PAD = 8
LIMIT = 8 << 20
bf16, f32 = jnp.bfloat16, jnp.float32
VMEM = pl.BlockSpec(memory_space=pltpu.VMEM)


def interpolate_kernel(fields, bracket, fraction, *refs, levels, order):
    *messages, flat, totals, near_fields, near_bracket, near_fraction, sem = refs
    places = [(message, i) for message in messages for i in range(message.shape[0])]
    groups, variables = fields.shape[:2]
    plev = bracket.shape[1]
    pairs = variables * plev
    step = levels // plev
    chunks = max(n for n in range(1, CHUNKS + 1) if (levels // 2) % n == 0)
    depth = levels // 2 // chunks

    def one_group(group):
        copies = [
            pltpu.make_async_copy(bracket.at[group], near_bracket.at[0], sem.at[chunks]),
            pltpu.make_async_copy(fraction.at[group], near_fraction.at[0], sem.at[chunks + 1]),
        ]
        copies += [
            pltpu.make_async_copy(
                fields.at[group, :, pl.ds(n * depth, depth)],
                near_fields.at[0, :, pl.ds(n * depth, depth)],
                sem.at[n],
            )
            for n in range(chunks)
        ]
        for copy in copies:
            copy.start()
        copies[0].wait()
        copies[1].wait()
        interpolate_group(group, copies[2:])

    def interpolate_group(group, arriving):
        for p in range(plev):
            base = min(p * step, levels - WINDOW)
            while arriving and (base + WINDOW) // 2 > depth * (chunks - len(arriving)):
                arriving.pop(0).wait()
            offset = near_bracket[0, p] - base
            index = jnp.concatenate([(offset + 1) >> 1, offset >> 1], 0).astype(f32).astype(bf16)
            high = index >= bf16(4)
            index = jnp.where(high, index - bf16(4), index)
            mid = index >= bf16(2)
            index = jnp.where(mid, index - bf16(2), index)
            low = index >= bf16(1)
            is_odd = (offset & 1) == 1
            weight = near_fraction[0, p].astype(f32)
            weight = jnp.where(is_odd, -weight, weight)
            for v in range(variables):
                w = [near_fields[0, v, base // 2 + k] for k in range(WINDOW // 2)]
                w = [jnp.where(low, w[k + 1], w[k]) for k in (0, 2, 4, 6)]
                w = [jnp.where(mid, w[k + 1], w[k]) for k in (0, 2)]
                picked = jnp.where(high, w[1], w[0]).astype(f32)
                even, odd = picked[:SUBLANES], picked[SUBLANES:]
                value = jnp.where(is_odd, odd, even) + weight * (odd - even)
                flat[pl.ds(v * plev + p, SUBLANES, stride=pairs + PAD), :] = value
        ones = jnp.ones((SUBLANES, flat.shape[1]), bf16)
        for r in range(SUBLANES):
            row = r
            if order:
                row = jnp.bitwise_xor(lax.axis_index("lon"), order[r])
            start = row * (pairs + PAD) if order is None else pl.multiple_of(row * (pairs + PAD), 8)
            block = flat[pl.ds(start, pairs), :].astype(bf16)
            if groups == 1:
                message, i = places[r]
                message[i, :pairs, :] = block
            else:
                messages[0][group * SUBLANES + r, :pairs, :] = block
            total = lax.dot_general(ones, block, (((1,), (1,)), ((), ())), preferred_element_type=f32)
            totals[group, pl.ds(row, 1)] = total[:1]

    if groups == 1:
        one_group(0)
    else:
        pl.loop(0, groups)(one_group)
    sums = totals[...].reshape(groups * SUBLANES, pairs)
    main = sums.astype(bf16)
    both = jnp.concatenate([main, (sums - main.astype(f32)).astype(bf16)], 0)
    for message, i in places:
        message[i, pairs:, :] = both


def interpolate(fields, bracket, fraction, sizes, order):
    variables, levels, rows, columns = fields.shape
    plev = bracket.shape[0]
    groups = rows // SUBLANES
    pairs = variables * plev
    assert rows % SUBLANES == 0 and levels % 2 == 0 and pairs == columns
    grouped = fields.reshape(variables, levels, groups, SUBLANES, columns).transpose(2, 0, 1, 3, 4)
    grouped = grouped.reshape(groups, variables, levels // 2, 2 * SUBLANES, columns)
    bracket = bracket.reshape(plev, groups, SUBLANES, columns).transpose(1, 0, 2, 3)
    fraction = fraction.reshape(plev, groups, SUBLANES, columns).transpose(1, 0, 2, 3)
    return pl.pallas_call(
        functools.partial(interpolate_kernel, levels=levels, order=order),
        out_shape=[jax.ShapeDtypeStruct((n, pairs + 2 * rows, columns), bf16) for n in sizes],
        in_specs=[pl.BlockSpec(memory_space=pltpu.HBM)] * 3,
        out_specs=[VMEM] * len(sizes),
        scratch_shapes=[
            pltpu.VMEM((SUBLANES * (pairs + PAD), columns), f32),
            pltpu.VMEM((groups, SUBLANES, pairs), f32),
            pltpu.VMEM((1,) + grouped.shape[1:], bf16),
            pltpu.VMEM((1,) + bracket.shape[1:], jnp.int32),
            pltpu.VMEM((1,) + fraction.shape[1:], bf16),
            pltpu.SemaphoreType.DMA((CHUNKS + 2,)),
        ],
        compiler_params=pltpu.CompilerParams(vmem_limit_bytes=LIMIT),
        name="interpolate",
    )(*(pltpu.with_memory_space_constraint(x, pltpu.HBM) for x in (grouped, bracket, fraction)))


def lay_kernel(*refs, pairs, parts):
    *blocks, whole, sem = refs
    columns = blocks[0].shape[-1]
    copies = []
    for j, (block, i, mask) in enumerate(parts):
        source = j if mask is None else jnp.bitwise_xor(lax.axis_index("lon"), mask)
        start = pl.multiple_of(source * columns, columns)
        copies.append(
            pltpu.make_async_copy(
                blocks[block].at[i, :pairs], whole.at[:, pl.ds(start, columns)], sem.at[j]
            )
        )
    for copy in copies:
        copy.start()
    for copy in copies:
        copy.wait()


def lay(blocks, parts, pairs):
    columns = blocks[0].shape[-1]
    anywhere = pl.BlockSpec(memory_space=pl.ANY)
    return pl.pallas_call(
        functools.partial(lay_kernel, pairs=pairs, parts=parts),
        out_shape=jax.ShapeDtypeStruct((pairs, len(parts) * columns), bf16),
        in_specs=[anywhere] * len(blocks),
        out_specs=anywhere,
        scratch_shapes=[pltpu.SemaphoreType.DMA((len(parts),))],
        compiler_params=pltpu.CompilerParams(vmem_limit_bytes=1 << 20),
        cost_estimate=pl.CostEstimate(
            flops=2 * pairs * len(parts) * columns * 1024,
            bytes_accessed=4 * pairs * len(parts) * columns,
            transcendentals=0,
        ),
        name="lay",
    )(*blocks)


def swap(value, mask):
    return lax.ppermute(value, "lon", [(i, i ^ mask) for i in range(lax.axis_size("lon"))])


def edge_routes(lon_count, lat_count):
    routes = []
    start = 1
    if lon_count == 8 and lat_count > 1:
        ring = [(0, 3), (1, 0), (1, 2), (1, 3), (0, 2), (0, 6)]
        routes += list(zip(ring, ring[1:] + ring[:1]))
        start = 2
    pairs = [((b, 0), (b - 1, 1)) for b in range(start, lat_count)]
    pairs += [((b, lon_count - 1), (b + 1, lon_count - 2)) for b in range(lat_count - 1)]
    taken = {place for pair in pairs + routes for place in pair}
    masks = [mask for mask in (1, 3, 5, 4) if mask < lon_count]
    masks += [mask for mask in range(1, lon_count) if mask not in masks]
    for b in range(lat_count):
        for j in range(lon_count):
            if (b, j) not in taken:
                other = next((b, j ^ mask) for mask in masks if (b, j ^ mask) not in taken)
                taken |= {(b, j), other}
                pairs.append(((b, j), other))
    routes += pairs + [(t, s) for s, t in pairs]
    return [(s[1] * lat_count + s[0], t[1] * lat_count + t[0]) for s, t in routes]


def exchange(fields, bracket, fraction):
    count = lax.axis_size("lon")
    if count != SUBLANES:
        (payload,) = interpolate(fields, bracket, fraction, [count], None)
        received = lax.all_to_all(payload, "lon", split_axis=0, concat_axis=0, tiled=True)
        return [received], [(0, j, None) for j in range(count)]
    order = [0, 1] + [mask ^ 1 for mask in BEFORE]
    sizes = [1, 1 + len(BEFORE)]
    for mask in AFTER:
        order += [mask, mask ^ 1]
        sizes.append(2)
    for mask in BEFORE:
        order.append(mask)
        sizes.append(1)
    mine, other, *messages = interpolate(fields, bracket, fraction, sizes, order)
    other = swap(other, 1)
    blocks, parts = [mine, other], [(0, 0, 0), (1, 0, 1)]
    for mask, message in zip(AFTER, messages):
        message = swap(message, mask)
        blocks += [message, swap(message[1:], 1)]
        parts += [(len(blocks) - 2, 0, mask), (len(blocks) - 1, 0, mask ^ 1)]
    for i, (mask, message) in enumerate(zip(BEFORE, messages[len(AFTER) :])):
        blocks.append(swap(jnp.concatenate([message, other[i + 1 : i + 2]], 0), mask))
        parts += [(len(blocks) - 1, 0, mask), (len(blocks) - 1, 1, mask ^ 1)]
    return blocks, parts


def shards(fields, bracket, fraction):
    variables, _, rows, columns = fields.shape
    plev = bracket.shape[0]
    pairs = variables * plev
    lon_count, lat_count = lax.axis_size("lon"), lax.axis_size("lat")
    lon_place, lat_place = lax.axis_index("lon"), lax.axis_index("lat")
    assert rows == lon_count

    blocks, parts = exchange(fields, bracket, fraction)

    if len(blocks) == 1:
        sums = jnp.sum(blocks[0][:, pairs:].astype(f32), 0)
    else:
        sums = sum(blocks[block][i, pairs:].astype(f32) for block, i, _ in parts)
    means = (sums[:rows] + sums[rows:]) / f32(lon_count * columns)
    first_place, last_place = lon_place == 0, lon_place == lon_count - 1

    edge = jnp.where(lon_place < lon_count // 2, means[rows - 1], means[0])
    beyond = lax.ppermute(edge, ("lon", "lat"), edge_routes(lon_count, lat_count))

    on_pressure = lay(blocks, parts, pairs)

    own = lax.dynamic_index_in_dim(means, lon_place, 0, False)
    below = lax.dynamic_index_in_dim(means, jnp.maximum(lon_place - 1, 0), 0, False)
    above = lax.dynamic_index_in_dim(means, jnp.minimum(lon_place + 1, rows - 1), 0, False)
    below = jnp.where(first_place, beyond, below)
    above = jnp.where(last_place, beyond, above)
    first_row = first_place & (lat_place == 0)
    last_row = last_place & (lat_place == lat_count - 1)
    meridional = jnp.where(
        first_row, above - own, jnp.where(last_row, own - below, 0.5 * (above - below))
    )
    return (
        on_pressure.reshape(variables, plev, 1, lon_count * columns),
        own.reshape(variables, plev, 1),
        meridional.reshape(variables, plev, 1),
    )


def solution(mesh):
    return jax.shard_map(
        shards,
        mesh=mesh,
        in_specs=(P(None, None, "lat", "lon"), P(None, "lat", "lon"), P(None, "lat", "lon")),
        out_specs=(
            P(None, None, ("lat", "lon"), None),
            P(None, None, ("lat", "lon")),
            P(None, None, ("lat", "lon")),
        ),
        check_vma=False,
    )
```

```python
import functools

import jax
import jax.numpy as jnp
from jax import lax
from jax.experimental import pallas as pl
from jax.experimental.pallas import tpu as pltpu
from jax.sharding import PartitionSpec as P

WINDOW = 16
AFTER = (7,)
BEFORE = (3, 5)
SUBLANES = 8
CHUNKS = 4
PAD = 8
LIMIT = 8 << 20
bf16, f32 = jnp.bfloat16, jnp.float32
VMEM = pl.BlockSpec(memory_space=pltpu.VMEM)


def interpolate_kernel(fields, bracket, fraction, *refs, levels, order):
    *messages, flat, sums, near_fields, near_bracket, near_fraction, sem = refs
    places = [(message, i) for message in messages for i in range(message.shape[0])]
    groups, variables = fields.shape[:2]
    plev = bracket.shape[1]
    pairs = variables * plev
    step = levels // plev
    chunks = max(n for n in range(1, CHUNKS + 1) if (levels // 2) % n == 0)
    depth = levels // 2 // chunks

    def one_group(group):
        copies = [
            pltpu.make_async_copy(bracket.at[group], near_bracket.at[0], sem.at[chunks]),
            pltpu.make_async_copy(fraction.at[group], near_fraction.at[0], sem.at[chunks + 1]),
        ]
        copies += [
            pltpu.make_async_copy(
                fields.at[group, :, pl.ds(n * depth, depth)],
                near_fields.at[0, :, pl.ds(n * depth, depth)],
                sem.at[n],
            )
            for n in range(chunks)
        ]
        for copy in copies:
            copy.start()
        copies[0].wait()
        copies[1].wait()
        interpolate_group(group, copies[2:])

    def interpolate_group(group, arriving):
        for p in range(plev):
            base = min(p * step, levels - WINDOW)
            while arriving and (base + WINDOW) // 2 > depth * (chunks - len(arriving)):
                arriving.pop(0).wait()
            offset = near_bracket[0, p] - base
            index = jnp.concatenate([(offset + 1) >> 1, offset >> 1], 0).astype(f32).astype(bf16)
            high = index >= bf16(4)
            index = jnp.where(high, index - bf16(4), index)
            mid = index >= bf16(2)
            index = jnp.where(mid, index - bf16(2), index)
            low = index >= bf16(1)
            is_odd = (offset & 1) == 1
            weight = near_fraction[0, p].astype(f32)
            weight = jnp.where(is_odd, -weight, weight)
            for v in range(variables):
                w = [near_fields[0, v, base // 2 + k] for k in range(WINDOW // 2)]
                w = [jnp.where(low, w[k + 1], w[k]) for k in (0, 2, 4, 6)]
                w = [jnp.where(mid, w[k + 1], w[k]) for k in (0, 2)]
                picked = jnp.where(high, w[1], w[0]).astype(f32)
                even, odd = picked[:SUBLANES], picked[SUBLANES:]
                value = jnp.where(is_odd, odd, even) + weight * (odd - even)
                flat[pl.ds(v * plev + p, SUBLANES, stride=pairs + PAD), :] = value
        ones = jnp.ones((SUBLANES, flat.shape[1]), bf16)
        for r in range(SUBLANES):
            row = r
            if order:
                row = jnp.bitwise_xor(lax.axis_index("lon"), order[r])
            start = row * (pairs + PAD) if order is None else pl.multiple_of(row * (pairs + PAD), 8)
            block = flat[pl.ds(start, pairs), :].astype(bf16)
            if groups == 1:
                message, i = places[r]
                message[i, :pairs, :] = block
            else:
                messages[0][group * SUBLANES + r, :pairs, :] = block
            total = lax.dot_general(ones, block, (((1,), (1,)), ((), ())), preferred_element_type=f32)
            sums[pl.ds(SUBLANES * (group + 1) + row, 1), :] = total[:1]

    edge = jnp.zeros((SUBLANES, pairs), f32)
    sums[:SUBLANES, :] = edge
    sums[SUBLANES * (groups + 1) :, :] = edge
    if groups == 1:
        one_group(0)
    else:
        pl.loop(0, groups)(one_group)
    rows = groups * SUBLANES
    last, first = sums[rows + SUBLANES - 1 : rows + SUBLANES, :], sums[SUBLANES : SUBLANES + 1, :]
    place = lax.broadcasted_iota(jnp.int32, (SUBLANES, pairs), 0)
    for r, (message, i) in enumerate(places):
        row = r if order is None else jnp.bitwise_xor(lax.axis_index("lon"), order[r])
        three, again = sums[pl.ds(row + SUBLANES - 1, SUBLANES), :], sums[pl.ds(row + SUBLANES - 5, SUBLANES), :]
        four = jnp.where(place < 4, three, again)
        four = jnp.where((place & 3) == 3, jnp.where(2 * row < rows, last, first), four)
        main = four.astype(bf16).astype(f32)
        message[i, pairs:, :] = jnp.where(place < 4, main, four - main).astype(bf16)


def interpolate(fields, bracket, fraction, sizes, order):
    variables, levels, rows, columns = fields.shape
    plev = bracket.shape[0]
    groups = rows // SUBLANES
    pairs = variables * plev
    assert rows % SUBLANES == 0 and levels % 2 == 0 and pairs == columns
    grouped = fields.reshape(variables, levels, groups, SUBLANES, columns).transpose(2, 0, 1, 3, 4)
    grouped = grouped.reshape(groups, variables, levels // 2, 2 * SUBLANES, columns)
    bracket = bracket.reshape(plev, groups, SUBLANES, columns).transpose(1, 0, 2, 3)
    fraction = fraction.reshape(plev, groups, SUBLANES, columns).transpose(1, 0, 2, 3)
    return pl.pallas_call(
        functools.partial(interpolate_kernel, levels=levels, order=order),
        out_shape=[jax.ShapeDtypeStruct((n, pairs + SUBLANES, columns), bf16) for n in sizes],
        in_specs=[pl.BlockSpec(memory_space=pltpu.HBM)] * 3,
        out_specs=[VMEM] * len(sizes),
        scratch_shapes=[
            pltpu.VMEM((SUBLANES * (pairs + PAD), columns), f32),
            pltpu.VMEM((rows + 2 * SUBLANES, pairs), f32),
            pltpu.VMEM((1,) + grouped.shape[1:], bf16),
            pltpu.VMEM((1,) + bracket.shape[1:], jnp.int32),
            pltpu.VMEM((1,) + fraction.shape[1:], bf16),
            pltpu.SemaphoreType.DMA((CHUNKS + 2,)),
        ],
        compiler_params=pltpu.CompilerParams(vmem_limit_bytes=LIMIT),
        name="interpolate",
    )(*(pltpu.with_memory_space_constraint(x, pltpu.HBM) for x in (grouped, bracket, fraction)))


def lay_kernel(*refs, pairs, parts):
    *blocks, whole, sem = refs
    columns = blocks[0].shape[-1]
    copies = []
    for j, (block, i, mask) in enumerate(parts):
        source = j if mask is None else jnp.bitwise_xor(lax.axis_index("lon"), mask)
        start = pl.multiple_of(source * columns, columns)
        copies.append(
            pltpu.make_async_copy(
                blocks[block].at[i, :pairs], whole.at[:, pl.ds(start, columns)], sem.at[j]
            )
        )
    for copy in copies:
        copy.start()
    for copy in copies:
        copy.wait()


def lay(blocks, parts, pairs):
    columns = blocks[0].shape[-1]
    anywhere = pl.BlockSpec(memory_space=pl.ANY)
    return pl.pallas_call(
        functools.partial(lay_kernel, pairs=pairs, parts=parts),
        out_shape=jax.ShapeDtypeStruct((pairs, len(parts) * columns), bf16),
        in_specs=[anywhere] * len(blocks),
        out_specs=anywhere,
        scratch_shapes=[pltpu.SemaphoreType.DMA((len(parts),))],
        compiler_params=pltpu.CompilerParams(vmem_limit_bytes=1 << 20),
        cost_estimate=pl.CostEstimate(
            flops=2 * pairs * len(parts) * columns * 1024,
            bytes_accessed=4 * pairs * len(parts) * columns,
            transcendentals=0,
        ),
        name="lay",
    )(*blocks)


def swap(value, mask):
    return lax.ppermute(value, "lon", [(i, i ^ mask) for i in range(lax.axis_size("lon"))])


def edge_routes(lon_count, lat_count):
    routes = []
    start = 1
    if lon_count == 8 and lat_count > 1:
        ring = [(0, 3), (1, 0), (1, 2), (1, 3), (0, 2), (0, 6)]
        routes += list(zip(ring, ring[1:] + ring[:1]))
        start = 2
    pairs = [((b, 0), (b - 1, 1)) for b in range(start, lat_count)]
    pairs += [((b, lon_count - 1), (b + 1, lon_count - 2)) for b in range(lat_count - 1)]
    taken = {place for pair in pairs + routes for place in pair}
    masks = [mask for mask in (1, 3, 5, 4) if mask < lon_count]
    masks += [mask for mask in range(1, lon_count) if mask not in masks]
    for b in range(lat_count):
        for j in range(lon_count):
            if (b, j) not in taken:
                other = next((b, j ^ mask) for mask in masks if (b, j ^ mask) not in taken)
                taken |= {(b, j), other}
                pairs.append(((b, j), other))
    routes += pairs + [(t, s) for s, t in pairs]
    return [(s[1] * lat_count + s[0], t[1] * lat_count + t[0]) for s, t in routes]


def exchange(fields, bracket, fraction):
    count = lax.axis_size("lon")
    if count != SUBLANES:
        (payload,) = interpolate(fields, bracket, fraction, [count], None)
        received = lax.all_to_all(payload, "lon", split_axis=0, concat_axis=0, tiled=True)
        return [received], [(0, j, None) for j in range(count)]
    order = [0, 1] + [mask ^ 1 for mask in BEFORE]
    sizes = [1, 1 + len(BEFORE)]
    for mask in AFTER:
        order += [mask, mask ^ 1]
        sizes.append(2)
    for mask in BEFORE:
        order.append(mask)
        sizes.append(1)
    mine, other, *messages = interpolate(fields, bracket, fraction, sizes, order)
    other = swap(other, 1)
    blocks, parts = [mine, other], [(0, 0, 0), (1, 0, 1)]
    for mask, message in zip(AFTER, messages):
        message = swap(message, mask)
        blocks += [message, swap(message[1:], 1)]
        parts += [(len(blocks) - 2, 0, mask), (len(blocks) - 1, 0, mask ^ 1)]
    for i, (mask, message) in enumerate(zip(BEFORE, messages[len(AFTER) :])):
        blocks.append(swap(jnp.concatenate([message, other[i + 1 : i + 2]], 0), mask))
        parts += [(len(blocks) - 1, 0, mask), (len(blocks) - 1, 1, mask ^ 1)]
    return blocks, parts


def shards(fields, bracket, fraction):
    variables, _, rows, columns = fields.shape
    plev = bracket.shape[0]
    pairs = variables * plev
    lon_count, lat_count = lax.axis_size("lon"), lax.axis_size("lat")
    lon_place, lat_place = lax.axis_index("lon"), lax.axis_index("lat")
    assert rows == lon_count

    blocks, parts = exchange(fields, bracket, fraction)

    if len(blocks) == 1:
        sums = jnp.sum(blocks[0][:, pairs:].astype(f32), 0)
    else:
        sums = sum(blocks[block][i, pairs:].astype(f32) for block, i, _ in parts)
    below, own, above, far = (sums[:4] + sums[4:]) / f32(lon_count * columns)
    first_place, last_place = lon_place == 0, lon_place == lon_count - 1

    beyond = lax.ppermute(far, ("lon", "lat"), edge_routes(lon_count, lat_count))

    on_pressure = lay(blocks, parts, pairs)

    below = jnp.where(first_place, beyond, below)
    above = jnp.where(last_place, beyond, above)
    first_row = first_place & (lat_place == 0)
    last_row = last_place & (lat_place == lat_count - 1)
    meridional = jnp.where(
        first_row, above - own, jnp.where(last_row, own - below, 0.5 * (above - below))
    )
    return (
        on_pressure.reshape(variables, plev, 1, lon_count * columns),
        own.reshape(variables, plev, 1),
        meridional.reshape(variables, plev, 1),
    )


def solution(mesh):
    return jax.shard_map(
        shards,
        mesh=mesh,
        in_specs=(P(None, None, "lat", "lon"), P(None, "lat", "lon"), P(None, "lat", "lon")),
        out_specs=(
            P(None, None, ("lat", "lon"), None),
            P(None, None, ("lat", "lon")),
            P(None, None, ("lat", "lon")),
        ),
        check_vma=False,
    )
```

```python
import functools

import jax
import jax.numpy as jnp
from jax import lax
from jax.experimental import pallas as pl
from jax.experimental.pallas import tpu as pltpu
from jax.sharding import PartitionSpec as P

WINDOW = 16
AFTER = (7,)
BEFORE = (3, 5)
SUBLANES = 8
CHUNKS = 4
PAD = 8
LIMIT = 8 << 20
bf16, f32 = jnp.bfloat16, jnp.float32
VMEM = pl.BlockSpec(memory_space=pltpu.VMEM)


def interpolate_kernel(fields, bracket, fraction, *refs, levels, order):
    *messages, flat, sums, near_fields, near_bracket, near_fraction, sem = refs
    places = [(message, i) for message in messages for i in range(message.shape[0])]
    groups, variables = fields.shape[:2]
    plev = bracket.shape[1]
    pairs = variables * plev
    step = levels // plev
    chunks = max(n for n in range(1, CHUNKS + 1) if (levels // 2) % n == 0)
    depth = levels // 2 // chunks

    def one_group(group):
        copies = [
            pltpu.make_async_copy(bracket.at[group], near_bracket.at[0], sem.at[chunks]),
            pltpu.make_async_copy(fraction.at[group], near_fraction.at[0], sem.at[chunks + 1]),
        ]
        copies += [
            pltpu.make_async_copy(
                fields.at[group, :, pl.ds(n * depth, depth)],
                near_fields.at[0, :, pl.ds(n * depth, depth)],
                sem.at[n],
            )
            for n in range(chunks)
        ]
        for copy in copies:
            copy.start()
        copies[0].wait()
        copies[1].wait()
        interpolate_group(group, copies[2:])

    def interpolate_group(group, arriving):
        for p in range(plev):
            base = min(p * step, levels - WINDOW)
            while arriving and (base + WINDOW) // 2 > depth * (chunks - len(arriving)):
                arriving.pop(0).wait()
            offset = near_bracket[0, p] - base
            index = jnp.concatenate([(offset + 1) >> 1, offset >> 1], 0).astype(f32).astype(bf16)
            high = index >= bf16(4)
            index = jnp.where(high, index - bf16(4), index)
            mid = index >= bf16(2)
            index = jnp.where(mid, index - bf16(2), index)
            low = index >= bf16(1)
            is_odd = (offset & 1) == 1
            weight = near_fraction[0, p].astype(f32)
            weight = jnp.where(is_odd, -weight, weight)
            for v in range(variables):
                w = [near_fields[0, v, base // 2 + k] for k in range(WINDOW // 2)]
                w = [jnp.where(low, w[k + 1], w[k]) for k in (0, 2, 4, 6)]
                w = [jnp.where(mid, w[k + 1], w[k]) for k in (0, 2)]
                picked = jnp.where(high, w[1], w[0]).astype(f32)
                even, odd = picked[:SUBLANES], picked[SUBLANES:]
                value = jnp.where(is_odd, odd, even) + weight * (odd - even)
                flat[pl.ds(v * plev + p, SUBLANES, stride=pairs + PAD), :] = value
        ones = jnp.ones((SUBLANES, flat.shape[1]), bf16)
        for r in range(SUBLANES):
            row = r
            if order:
                row = jnp.bitwise_xor(lax.axis_index("lon"), order[r])
            start = row * (pairs + PAD) if order is None else pl.multiple_of(row * (pairs + PAD), 8)
            block = flat[pl.ds(start, pairs), :].astype(bf16)
            if groups == 1:
                message, i = places[r]
                message[i, :pairs, :] = block
            else:
                messages[0][group * SUBLANES + r, :pairs, :] = block
            total = lax.dot_general(ones, block, (((1,), (1,)), ((), ())), preferred_element_type=f32)
            sums[pl.ds(SUBLANES * (group + 1) + row, 1), :] = total[:1]

    edge = jnp.zeros((SUBLANES, pairs), f32)
    sums[:SUBLANES, :] = edge
    sums[SUBLANES * (groups + 1) :, :] = edge
    if groups == 1:
        one_group(0)
    else:
        pl.loop(0, groups)(one_group)
    rows = groups * SUBLANES
    last, first = sums[rows + SUBLANES - 1 : rows + SUBLANES, :], sums[SUBLANES : SUBLANES + 1, :]
    place = lax.broadcasted_iota(jnp.int32, (SUBLANES, pairs), 0)
    for r, (message, i) in enumerate(places):
        row = r if order is None else jnp.bitwise_xor(lax.axis_index("lon"), order[r])
        three, again = sums[pl.ds(row + SUBLANES - 1, SUBLANES), :], sums[pl.ds(row + SUBLANES - 5, SUBLANES), :]
        four = jnp.where(place < 4, three, again)
        four = jnp.where((place & 3) == 3, jnp.where(2 * row < rows, last, first), four)
        main = four.astype(bf16).astype(f32)
        message[i, pairs:, :] = jnp.where(place < 4, main, four - main).astype(bf16)


def interpolate(fields, bracket, fraction, sizes, order):
    variables, levels, rows, columns = fields.shape
    plev = bracket.shape[0]
    groups = rows // SUBLANES
    pairs = variables * plev
    assert rows % SUBLANES == 0 and levels % 2 == 0 and pairs == columns
    grouped = fields.reshape(variables, levels, groups, SUBLANES, columns).transpose(2, 0, 1, 3, 4)
    grouped = grouped.reshape(groups, variables, levels // 2, 2 * SUBLANES, columns)
    bracket = bracket.reshape(plev, groups, SUBLANES, columns).transpose(1, 0, 2, 3)
    fraction = fraction.reshape(plev, groups, SUBLANES, columns).transpose(1, 0, 2, 3)
    return pl.pallas_call(
        functools.partial(interpolate_kernel, levels=levels, order=order),
        out_shape=[jax.ShapeDtypeStruct((n, pairs + SUBLANES, columns), bf16) for n in sizes],
        in_specs=[pl.BlockSpec(memory_space=pltpu.HBM)] * 3,
        out_specs=[VMEM] * len(sizes),
        scratch_shapes=[
            pltpu.VMEM((SUBLANES * (pairs + PAD), columns), f32),
            pltpu.VMEM((rows + 2 * SUBLANES, pairs), f32),
            pltpu.VMEM((1,) + grouped.shape[1:], bf16),
            pltpu.VMEM((1,) + bracket.shape[1:], jnp.int32),
            pltpu.VMEM((1,) + fraction.shape[1:], bf16),
            pltpu.SemaphoreType.DMA((CHUNKS + 2,)),
        ],
        compiler_params=pltpu.CompilerParams(vmem_limit_bytes=LIMIT),
        name="interpolate",
    )(*(pltpu.with_memory_space_constraint(x, pltpu.HBM) for x in (grouped, bracket, fraction)))


def lay_kernel(*refs, pairs, parts):
    *blocks, whole, sem = refs
    columns = blocks[0].shape[-1]
    copies = []
    for j, (block, i, mask) in enumerate(parts):
        source = j if mask is None else jnp.bitwise_xor(lax.axis_index("lon"), mask)
        start = pl.multiple_of(source * columns, columns)
        copies.append(
            pltpu.make_async_copy(
                blocks[block].at[i, :pairs], whole.at[:, pl.ds(start, columns)], sem.at[j]
            )
        )
    for copy in copies:
        copy.start()
    for copy in copies:
        copy.wait()


def lay(blocks, parts, pairs):
    columns = blocks[0].shape[-1]
    anywhere = pl.BlockSpec(memory_space=pl.ANY)
    return pl.pallas_call(
        functools.partial(lay_kernel, pairs=pairs, parts=parts),
        out_shape=jax.ShapeDtypeStruct((pairs, len(parts) * columns), bf16),
        in_specs=[anywhere] * len(blocks),
        out_specs=anywhere,
        scratch_shapes=[pltpu.SemaphoreType.DMA((len(parts),))],
        compiler_params=pltpu.CompilerParams(vmem_limit_bytes=1 << 20),
        cost_estimate=pl.CostEstimate(
            flops=2 * pairs * len(parts) * columns * 1024,
            bytes_accessed=4 * pairs * len(parts) * columns,
            transcendentals=0,
        ),
        name="lay",
    )(*blocks)


def swap(value, mask):
    return lax.ppermute(value, "lon", [(i, i ^ mask) for i in range(lax.axis_size("lon"))])


def edge_routes(lon_count, lat_count):
    routes = []
    start = 1
    if lon_count == 8 and lat_count > 1:
        ring = [(0, 3), (1, 0), (1, 3), (1, 2), (0, 2), (0, 6)]
        routes += list(zip(ring, ring[1:] + ring[:1]))
        start = 2
    pairs = [((b, 0), (b - 1, 1)) for b in range(start, lat_count)]
    pairs += [((b, lon_count - 1), (b + 1, lon_count - 2)) for b in range(lat_count - 1)]
    taken = {place for pair in pairs + routes for place in pair}
    masks = [mask for mask in (1, 3, 5, 4) if mask < lon_count]
    masks += [mask for mask in range(1, lon_count) if mask not in masks]
    for b in range(lat_count):
        for j in range(lon_count):
            if (b, j) not in taken:
                other = next((b, j ^ mask) for mask in masks if (b, j ^ mask) not in taken)
                taken |= {(b, j), other}
                pairs.append(((b, j), other))
    routes += pairs + [(t, s) for s, t in pairs]
    return [(s[1] * lat_count + s[0], t[1] * lat_count + t[0]) for s, t in routes]


def exchange(fields, bracket, fraction):
    count = lax.axis_size("lon")
    if count != SUBLANES:
        (payload,) = interpolate(fields, bracket, fraction, [count], None)
        received = lax.all_to_all(payload, "lon", split_axis=0, concat_axis=0, tiled=True)
        return [received], [(0, j, None) for j in range(count)]
    order = [0, 1] + [mask ^ 1 for mask in BEFORE]
    sizes = [1, 1 + len(BEFORE)]
    for mask in AFTER:
        order += [mask, mask ^ 1]
        sizes.append(2)
    for mask in BEFORE:
        order.append(mask)
        sizes.append(1)
    mine, other, *messages = interpolate(fields, bracket, fraction, sizes, order)
    other = swap(other, 1)
    blocks, parts = [mine, other], [(0, 0, 0), (1, 0, 1)]
    for mask, message in zip(AFTER, messages):
        message = swap(message, mask)
        blocks += [message, swap(message[1:], 1)]
        parts += [(len(blocks) - 2, 0, mask), (len(blocks) - 1, 0, mask ^ 1)]
    for i, (mask, message) in enumerate(zip(BEFORE, messages[len(AFTER) :])):
        blocks.append(swap(jnp.concatenate([message, other[i + 1 : i + 2]], 0), mask))
        parts += [(len(blocks) - 1, 0, mask), (len(blocks) - 1, 1, mask ^ 1)]
    return blocks, parts


def finish_kernel(own, meridional, zonal_out, meridional_out):
    variables, _, plev = zonal_out.shape
    for v in range(variables):
        zonal_out[v] = own[:, v * plev : (v + 1) * plev]
        meridional_out[v] = meridional[:, v * plev : (v + 1) * plev]


def finish(own, meridional, variables):
    out = jax.ShapeDtypeStruct((variables, 1, own.shape[0] // variables), f32)
    return pl.pallas_call(
        finish_kernel,
        out_shape=[out, out],
        in_specs=[VMEM] * 2,
        out_specs=[VMEM] * 2,
        compiler_params=pltpu.CompilerParams(vmem_limit_bytes=1 << 20),
        name="finish",
    )(own[None], meridional[None])


def shards(fields, bracket, fraction):
    variables, _, rows, columns = fields.shape
    plev = bracket.shape[0]
    pairs = variables * plev
    lon_count, lat_count = lax.axis_size("lon"), lax.axis_size("lat")
    lon_place, lat_place = lax.axis_index("lon"), lax.axis_index("lat")
    assert rows == lon_count

    blocks, parts = exchange(fields, bracket, fraction)

    if len(blocks) == 1:
        sums = jnp.sum(blocks[0][:, pairs:].astype(f32), 0)
    else:
        sums = sum(blocks[block][i, pairs:].astype(f32) for block, i, _ in parts)
    below, own, above, far = (sums[:4] + sums[4:]) / f32(lon_count * columns)
    first_place, last_place = lon_place == 0, lon_place == lon_count - 1

    beyond = lax.ppermute(far, ("lon", "lat"), edge_routes(lon_count, lat_count))

    on_pressure = lay(blocks, parts, pairs)

    below = jnp.where(first_place, beyond, below)
    above = jnp.where(last_place, beyond, above)
    first_row = first_place & (lat_place == 0)
    last_row = last_place & (lat_place == lat_count - 1)
    meridional = jnp.where(
        first_row, above - own, jnp.where(last_row, own - below, 0.5 * (above - below))
    )
    own, meridional = finish(own, meridional, variables)
    return (
        on_pressure.reshape(variables, plev, 1, lon_count * columns),
        own.reshape(variables, plev, 1),
        meridional.reshape(variables, plev, 1),
    )


def solution(mesh):
    return jax.shard_map(
        shards,
        mesh=mesh,
        in_specs=(P(None, None, "lat", "lon"), P(None, "lat", "lon"), P(None, "lat", "lon")),
        out_specs=(
            P(None, None, ("lat", "lon"), None),
            P(None, None, ("lat", "lon")),
            P(None, None, ("lat", "lon")),
        ),
        check_vma=False,
    )
```

```python
import functools

import jax
import jax.numpy as jnp
from jax import lax
from jax.experimental import pallas as pl
from jax.experimental.pallas import tpu as pltpu
from jax.sharding import PartitionSpec as P

WINDOW = 16
AFTER = (7,)
BEFORE = (3, 5)
SUBLANES = 8
CHUNKS = 4
PAD = 8
LIMIT = 8 << 20
bf16, f32 = jnp.bfloat16, jnp.float32
VMEM = pl.BlockSpec(memory_space=pltpu.VMEM)


def interpolate_kernel(fields, bracket, fraction, *refs, levels, order):
    *messages, flat, sums, near_fields, near_bracket, near_fraction, sem = refs
    places = [(message, i) for message in messages for i in range(message.shape[0])]
    groups, variables = fields.shape[:2]
    plev = bracket.shape[1]
    pairs = variables * plev
    step = levels // plev
    chunks = max(n for n in range(1, CHUNKS + 1) if (levels // 2) % n == 0)
    depth = levels // 2 // chunks

    def one_group(group):
        copies = [
            pltpu.make_async_copy(bracket.at[group], near_bracket.at[0], sem.at[chunks]),
            pltpu.make_async_copy(fraction.at[group], near_fraction.at[0], sem.at[chunks + 1]),
        ]
        copies += [
            pltpu.make_async_copy(
                fields.at[group, :, pl.ds(n * depth, depth)],
                near_fields.at[0, :, pl.ds(n * depth, depth)],
                sem.at[n],
            )
            for n in range(chunks)
        ]
        for copy in copies:
            copy.start()
        copies[0].wait()
        copies[1].wait()
        interpolate_group(group, copies[2:])

    def interpolate_group(group, arriving):
        for p in range(plev):
            base = min(p * step, levels - WINDOW)
            while arriving and (base + WINDOW) // 2 > depth * (chunks - len(arriving)):
                arriving.pop(0).wait()
            offset = near_bracket[0, p] - base
            index = jnp.concatenate([(offset + 1) >> 1, offset >> 1], 0).astype(f32).astype(bf16)
            high = index >= bf16(4)
            index = jnp.where(high, index - bf16(4), index)
            mid = index >= bf16(2)
            index = jnp.where(mid, index - bf16(2), index)
            low = index >= bf16(1)
            is_odd = (offset & 1) == 1
            weight = near_fraction[0, p].astype(f32)
            weight = jnp.where(is_odd, -weight, weight)
            for v in range(variables):
                w = [near_fields[0, v, base // 2 + k] for k in range(WINDOW // 2)]
                w = [jnp.where(low, w[k + 1], w[k]) for k in (0, 2, 4, 6)]
                w = [jnp.where(mid, w[k + 1], w[k]) for k in (0, 2)]
                picked = jnp.where(high, w[1], w[0]).astype(f32)
                even, odd = picked[:SUBLANES], picked[SUBLANES:]
                value = jnp.where(is_odd, odd, even) + weight * (odd - even)
                flat[pl.ds(v * plev + p, SUBLANES, stride=pairs + PAD), :] = value
        ones = jnp.ones((SUBLANES, flat.shape[1]), bf16)
        for r in range(SUBLANES):
            row = r
            if order:
                row = jnp.bitwise_xor(lax.axis_index("lon"), order[r])
            start = row * (pairs + PAD) if order is None else pl.multiple_of(row * (pairs + PAD), 8)
            block = flat[pl.ds(start, pairs), :].astype(bf16)
            if groups == 1:
                message, i = places[r]
                message[i, :pairs, :] = block
            else:
                messages[0][group * SUBLANES + r, :pairs, :] = block
            total = lax.dot_general(ones, block, (((1,), (1,)), ((), ())), preferred_element_type=f32)
            sums[pl.ds(SUBLANES * (group + 1) + row, 1), :] = total[:1]

    edge = jnp.zeros((SUBLANES, pairs), f32)
    sums[:SUBLANES, :] = edge
    sums[SUBLANES * (groups + 1) :, :] = edge
    if groups == 1:
        one_group(0)
    else:
        pl.loop(0, groups)(one_group)
    rows = groups * SUBLANES
    last, first = sums[rows + SUBLANES - 1 : rows + SUBLANES, :], sums[SUBLANES : SUBLANES + 1, :]
    place = lax.broadcasted_iota(jnp.int32, (SUBLANES, pairs), 0)
    for r, (message, i) in enumerate(places):
        row = r if order is None else jnp.bitwise_xor(lax.axis_index("lon"), order[r])
        three, again = sums[pl.ds(row + SUBLANES - 1, SUBLANES), :], sums[pl.ds(row + SUBLANES - 5, SUBLANES), :]
        four = jnp.where(place < 4, three, again)
        four = jnp.where((place & 3) == 3, jnp.where(2 * row < rows, last, first), four)
        main = four.astype(bf16).astype(f32)
        message[i, pairs:, :] = jnp.where(place < 4, main, four - main).astype(bf16)


def interpolate(fields, bracket, fraction, sizes, order):
    variables, levels, rows, columns = fields.shape
    plev = bracket.shape[0]
    groups = rows // SUBLANES
    pairs = variables * plev
    assert rows % SUBLANES == 0 and levels % 2 == 0 and pairs == columns
    grouped = fields.reshape(variables, levels, groups, SUBLANES, columns).transpose(2, 0, 1, 3, 4)
    grouped = grouped.reshape(groups, variables, levels // 2, 2 * SUBLANES, columns)
    bracket = bracket.reshape(plev, groups, SUBLANES, columns).transpose(1, 0, 2, 3)
    fraction = fraction.reshape(plev, groups, SUBLANES, columns).transpose(1, 0, 2, 3)
    return pl.pallas_call(
        functools.partial(interpolate_kernel, levels=levels, order=order),
        out_shape=[jax.ShapeDtypeStruct((n, pairs + SUBLANES, columns), bf16) for n in sizes],
        in_specs=[pl.BlockSpec(memory_space=pltpu.HBM)] * 3,
        out_specs=[VMEM] * len(sizes),
        scratch_shapes=[
            pltpu.VMEM((SUBLANES * (pairs + PAD), columns), f32),
            pltpu.VMEM((rows + 2 * SUBLANES, pairs), f32),
            pltpu.VMEM((1,) + grouped.shape[1:], bf16),
            pltpu.VMEM((1,) + bracket.shape[1:], jnp.int32),
            pltpu.VMEM((1,) + fraction.shape[1:], bf16),
            pltpu.SemaphoreType.DMA((CHUNKS + 2,)),
        ],
        compiler_params=pltpu.CompilerParams(vmem_limit_bytes=LIMIT),
        name="interpolate",
    )(*(pltpu.with_memory_space_constraint(x, pltpu.HBM) for x in (grouped, bracket, fraction)))


def lay_kernel(*refs, pairs, parts):
    *blocks, whole, sem = refs
    columns = blocks[0].shape[-1]
    copies = []
    for j, (block, i, mask) in enumerate(parts):
        source = j if mask is None else jnp.bitwise_xor(lax.axis_index("lon"), mask)
        start = pl.multiple_of(source * columns, columns)
        copies.append(
            pltpu.make_async_copy(
                blocks[block].at[i, :pairs], whole.at[:, pl.ds(start, columns)], sem.at[j]
            )
        )
    for copy in copies:
        copy.start()
    for copy in copies:
        copy.wait()


def lay(blocks, parts, pairs):
    columns = blocks[0].shape[-1]
    anywhere = pl.BlockSpec(memory_space=pl.ANY)
    return pl.pallas_call(
        functools.partial(lay_kernel, pairs=pairs, parts=parts),
        out_shape=jax.ShapeDtypeStruct((pairs, len(parts) * columns), bf16),
        in_specs=[anywhere] * len(blocks),
        out_specs=anywhere,
        scratch_shapes=[pltpu.SemaphoreType.DMA((len(parts),))],
        compiler_params=pltpu.CompilerParams(vmem_limit_bytes=1 << 20),
        cost_estimate=pl.CostEstimate(
            flops=2 * pairs * len(parts) * columns * 1024,
            bytes_accessed=4 * pairs * len(parts) * columns,
            transcendentals=0,
        ),
        name="lay",
    )(*blocks)


def swap(value, mask):
    return lax.ppermute(value, "lon", [(i, i ^ mask) for i in range(lax.axis_size("lon"))])


def edge_routes(lon_count, lat_count):
    routes, pairs = [], []
    if lon_count == 8 and lat_count > 1:
        top = lat_count - 1
        ring = [(0, 3)] + [(b, j) for b in range(1, lat_count) for j in (0, 1)] + [(top, 7), (top, 6)]
        ring += [(b, j) for b in reversed(range(top)) for j in (7, 6)] + [(0, 2)]
        routes += list(zip(ring, ring[1:] + ring[:1]))
    else:
        pairs += [((b, 0), (b - 1, 1)) for b in range(1, lat_count)]
        pairs += [((b, lon_count - 1), (b + 1, lon_count - 2)) for b in range(lat_count - 1)]
    taken = {place for pair in pairs + routes for place in pair}
    masks = [mask for mask in (1, 3, 5, 4) if mask < lon_count]
    masks += [mask for mask in range(1, lon_count) if mask not in masks]
    for b in range(lat_count):
        for j in range(lon_count):
            if (b, j) not in taken:
                other = next((b, j ^ mask) for mask in masks if (b, j ^ mask) not in taken)
                taken |= {(b, j), other}
                pairs.append(((b, j), other))
    routes += pairs + [(t, s) for s, t in pairs]
    return [(s[1] * lat_count + s[0], t[1] * lat_count + t[0]) for s, t in routes]


def exchange(fields, bracket, fraction):
    count = lax.axis_size("lon")
    if count != SUBLANES:
        (payload,) = interpolate(fields, bracket, fraction, [count], None)
        received = lax.all_to_all(payload, "lon", split_axis=0, concat_axis=0, tiled=True)
        return [received], [(0, j, None) for j in range(count)]
    order = [0, 1] + [mask ^ 1 for mask in BEFORE]
    sizes = [1, 1 + len(BEFORE)]
    for mask in AFTER:
        order += [mask, mask ^ 1]
        sizes.append(2)
    for mask in BEFORE:
        order.append(mask)
        sizes.append(1)
    mine, other, *messages = interpolate(fields, bracket, fraction, sizes, order)
    other = swap(other, 1)
    blocks, parts = [mine, other], [(0, 0, 0), (1, 0, 1)]
    for mask, message in zip(AFTER, messages):
        message = swap(message, mask)
        blocks += [message, swap(message[1:], 1)]
        parts += [(len(blocks) - 2, 0, mask), (len(blocks) - 1, 0, mask ^ 1)]
    for i, (mask, message) in enumerate(zip(BEFORE, messages[len(AFTER) :])):
        blocks.append(swap(jnp.concatenate([message, other[i + 1 : i + 2]], 0), mask))
        parts += [(len(blocks) - 1, 0, mask), (len(blocks) - 1, 1, mask ^ 1)]
    return blocks, parts


def finish_kernel(own, meridional, zonal_out, meridional_out):
    variables, _, plev = zonal_out.shape
    for v in range(variables):
        zonal_out[v] = own[:, v * plev : (v + 1) * plev]
        meridional_out[v] = meridional[:, v * plev : (v + 1) * plev]


def finish(own, meridional, variables):
    out = jax.ShapeDtypeStruct((variables, 1, own.shape[0] // variables), f32)
    return pl.pallas_call(
        finish_kernel,
        out_shape=[out, out],
        in_specs=[VMEM] * 2,
        out_specs=[VMEM] * 2,
        compiler_params=pltpu.CompilerParams(vmem_limit_bytes=1 << 20),
        name="finish",
    )(own[None], meridional[None])


def shards(fields, bracket, fraction):
    variables, _, rows, columns = fields.shape
    plev = bracket.shape[0]
    pairs = variables * plev
    lon_count, lat_count = lax.axis_size("lon"), lax.axis_size("lat")
    lon_place, lat_place = lax.axis_index("lon"), lax.axis_index("lat")
    assert rows == lon_count

    blocks, parts = exchange(fields, bracket, fraction)

    if len(blocks) == 1:
        sums = jnp.sum(blocks[0][:, pairs:].astype(f32), 0)
    else:
        sums = sum(blocks[block][i, pairs:].astype(f32) for block, i, _ in parts)
    below, own, above, far = (sums[:4] + sums[4:]) / f32(lon_count * columns)
    first_place, last_place = lon_place == 0, lon_place == lon_count - 1

    beyond = lax.ppermute(far, ("lon", "lat"), edge_routes(lon_count, lat_count))

    on_pressure = lay(blocks, parts, pairs)

    below = jnp.where(first_place, beyond, below)
    above = jnp.where(last_place, beyond, above)
    first_row = first_place & (lat_place == 0)
    last_row = last_place & (lat_place == lat_count - 1)
    meridional = jnp.where(
        first_row, above - own, jnp.where(last_row, own - below, 0.5 * (above - below))
    )
    own, meridional = finish(own, meridional, variables)
    return (
        on_pressure.reshape(variables, plev, 1, lon_count * columns),
        own.reshape(variables, plev, 1),
        meridional.reshape(variables, plev, 1),
    )


def solution(mesh):
    return jax.shard_map(
        shards,
        mesh=mesh,
        in_specs=(P(None, None, "lat", "lon"), P(None, "lat", "lon"), P(None, "lat", "lon")),
        out_specs=(
            P(None, None, ("lat", "lon"), None),
            P(None, None, ("lat", "lon")),
            P(None, None, ("lat", "lon")),
        ),
        check_vma=False,
    )
```

```python
import functools

import jax
import jax.numpy as jnp
from jax import lax
from jax.experimental import pallas as pl
from jax.experimental.pallas import tpu as pltpu
from jax.sharding import PartitionSpec as P

WINDOW = 16
AFTER = (7,)
BEFORE = (3, 5)
SUBLANES = 8
CHUNKS = 4
PAD = 8
PACKED = 16
LIMIT = 8 << 20
bf16, f32 = jnp.bfloat16, jnp.float32
VMEM = pl.BlockSpec(memory_space=pltpu.VMEM)


def interpolate_kernel(fields, bracket, fraction, *refs, levels, order):
    *messages, flat, sums, near_fields, near_bracket, near_fraction, sem = refs
    places = [(message, i) for message in messages for i in range(message.shape[0])]
    groups, variables = fields.shape[:2]
    plev = bracket.shape[1]
    pairs = variables * plev
    step = levels // plev
    chunks = max(n for n in range(1, CHUNKS + 1) if (levels // 2) % n == 0)
    depth = levels // 2 // chunks

    def one_group(group):
        copies = [
            pltpu.make_async_copy(bracket.at[group], near_bracket.at[0], sem.at[chunks]),
            pltpu.make_async_copy(fraction.at[group], near_fraction.at[0], sem.at[chunks + 1]),
        ]
        copies += [
            pltpu.make_async_copy(
                fields.at[group, :, pl.ds(n * depth, depth)],
                near_fields.at[0, :, pl.ds(n * depth, depth)],
                sem.at[n],
            )
            for n in range(chunks)
        ]
        for copy in copies:
            copy.start()
        copies[0].wait()
        copies[1].wait()
        interpolate_group(group, copies[2:])

    def interpolate_group(group, arriving):
        for p in range(plev):
            base = min(p * step, levels - WINDOW)
            while arriving and (base + WINDOW) // 2 > depth * (chunks - len(arriving)):
                arriving.pop(0).wait()
            offset = near_bracket[0, p] - base
            index = jnp.concatenate([(offset + 1) >> 1, offset >> 1], 0).astype(f32).astype(bf16)
            high = index >= bf16(4)
            index = jnp.where(high, index - bf16(4), index)
            mid = index >= bf16(2)
            index = jnp.where(mid, index - bf16(2), index)
            low = index >= bf16(1)
            is_odd = (offset & 1) == 1
            weight = near_fraction[0, p].astype(f32)
            weight = jnp.where(is_odd, -weight, weight)
            for v in range(variables):
                w = [near_fields[0, v, base // 2 + k] for k in range(WINDOW // 2)]
                w = [jnp.where(low, w[k + 1], w[k]) for k in (0, 2, 4, 6)]
                w = [jnp.where(mid, w[k + 1], w[k]) for k in (0, 2)]
                picked = jnp.where(high, w[1], w[0]).astype(f32)
                even, odd = picked[:SUBLANES], picked[SUBLANES:]
                value = jnp.where(is_odd, odd, even) + weight * (odd - even)
                flat[pl.ds(v * plev + p, SUBLANES, stride=pairs + PAD), :] = value
            if groups == 1 and (p + 1) % PACKED == 0:
                for r, (message, i) in enumerate(places):
                    row = r if order is None else jnp.bitwise_xor(lax.axis_index("lon"), order[r])
                    for v in range(variables):
                        at = v * plev + p + 1 - PACKED
                        start = pl.multiple_of(row * (pairs + PAD) + at, 8)
                        message[i, at : at + PACKED, :] = flat[pl.ds(start, PACKED), :].astype(bf16)
        ones = jnp.ones((SUBLANES, flat.shape[1]), bf16)
        for r in range(SUBLANES):
            row = r
            if order:
                row = jnp.bitwise_xor(lax.axis_index("lon"), order[r])
            start = row * (pairs + PAD) if order is None else pl.multiple_of(row * (pairs + PAD), 8)
            if groups == 1:
                message, i = places[r]
                block = message[i, :pairs, :]
            else:
                block = flat[pl.ds(start, pairs), :].astype(bf16)
                messages[0][group * SUBLANES + r, :pairs, :] = block
            total = lax.dot_general(ones, block, (((1,), (1,)), ((), ())), preferred_element_type=f32)
            sums[pl.ds(SUBLANES * (group + 1) + row, 1), :] = total[:1]

    edge = jnp.zeros((SUBLANES, pairs), f32)
    sums[:SUBLANES, :] = edge
    sums[SUBLANES * (groups + 1) :, :] = edge
    if groups == 1:
        one_group(0)
    else:
        pl.loop(0, groups)(one_group)
    rows = groups * SUBLANES
    last, first = sums[rows + SUBLANES - 1 : rows + SUBLANES, :], sums[SUBLANES : SUBLANES + 1, :]
    place = lax.broadcasted_iota(jnp.int32, (SUBLANES, pairs), 0)
    for r, (message, i) in enumerate(places):
        row = r if order is None else jnp.bitwise_xor(lax.axis_index("lon"), order[r])
        three, again = sums[pl.ds(row + SUBLANES - 1, SUBLANES), :], sums[pl.ds(row + SUBLANES - 5, SUBLANES), :]
        four = jnp.where(place < 4, three, again)
        four = jnp.where((place & 3) == 3, jnp.where(2 * row < rows, last, first), four)
        main = four.astype(bf16).astype(f32)
        message[i, pairs:, :] = jnp.where(place < 4, main, four - main).astype(bf16)


def interpolate(fields, bracket, fraction, sizes, order):
    variables, levels, rows, columns = fields.shape
    plev = bracket.shape[0]
    groups = rows // SUBLANES
    pairs = variables * plev
    assert rows % SUBLANES == 0 and levels % 2 == 0 and pairs == columns
    grouped = fields.reshape(variables, levels, groups, SUBLANES, columns).transpose(2, 0, 1, 3, 4)
    grouped = grouped.reshape(groups, variables, levels // 2, 2 * SUBLANES, columns)
    bracket = bracket.reshape(plev, groups, SUBLANES, columns).transpose(1, 0, 2, 3)
    fraction = fraction.reshape(plev, groups, SUBLANES, columns).transpose(1, 0, 2, 3)
    return pl.pallas_call(
        functools.partial(interpolate_kernel, levels=levels, order=order),
        out_shape=[jax.ShapeDtypeStruct((n, pairs + SUBLANES, columns), bf16) for n in sizes],
        in_specs=[pl.BlockSpec(memory_space=pltpu.HBM)] * 3,
        out_specs=[VMEM] * len(sizes),
        scratch_shapes=[
            pltpu.VMEM((SUBLANES * (pairs + PAD), columns), f32),
            pltpu.VMEM((rows + 2 * SUBLANES, pairs), f32),
            pltpu.VMEM((1,) + grouped.shape[1:], bf16),
            pltpu.VMEM((1,) + bracket.shape[1:], jnp.int32),
            pltpu.VMEM((1,) + fraction.shape[1:], bf16),
            pltpu.SemaphoreType.DMA((CHUNKS + 2,)),
        ],
        compiler_params=pltpu.CompilerParams(vmem_limit_bytes=LIMIT),
        name="interpolate",
    )(*(pltpu.with_memory_space_constraint(x, pltpu.HBM) for x in (grouped, bracket, fraction)))


def lay_kernel(*refs, pairs, parts):
    *blocks, whole, sem = refs
    columns = blocks[0].shape[-1]
    copies = []
    for j, (block, i, mask) in enumerate(parts):
        source = j if mask is None else jnp.bitwise_xor(lax.axis_index("lon"), mask)
        start = pl.multiple_of(source * columns, columns)
        copies.append(
            pltpu.make_async_copy(
                blocks[block].at[i, :pairs], whole.at[:, pl.ds(start, columns)], sem.at[j]
            )
        )
    for copy in copies:
        copy.start()
    for copy in copies:
        copy.wait()


def lay(blocks, parts, pairs):
    columns = blocks[0].shape[-1]
    anywhere = pl.BlockSpec(memory_space=pl.ANY)
    return pl.pallas_call(
        functools.partial(lay_kernel, pairs=pairs, parts=parts),
        out_shape=jax.ShapeDtypeStruct((pairs, len(parts) * columns), bf16),
        in_specs=[anywhere] * len(blocks),
        out_specs=anywhere,
        scratch_shapes=[pltpu.SemaphoreType.DMA((len(parts),))],
        compiler_params=pltpu.CompilerParams(vmem_limit_bytes=1 << 20),
        cost_estimate=pl.CostEstimate(
            flops=2 * pairs * len(parts) * columns * 1024,
            bytes_accessed=4 * pairs * len(parts) * columns,
            transcendentals=0,
        ),
        name="lay",
    )(*blocks)


def swap(value, mask):
    return lax.ppermute(value, "lon", [(i, i ^ mask) for i in range(lax.axis_size("lon"))])


def edge_routes(lon_count, lat_count):
    routes, pairs = [], []
    if lon_count == 8 and lat_count > 1:
        top = lat_count - 1
        ring = [(0, 3)] + [(b, j) for b in range(1, lat_count) for j in (0, 1)] + [(top, 7), (top, 6)]
        ring += [(b, j) for b in reversed(range(top)) for j in (7, 6)] + [(0, 2)]
        routes += list(zip(ring, ring[1:] + ring[:1]))
    else:
        pairs += [((b, 0), (b - 1, 1)) for b in range(1, lat_count)]
        pairs += [((b, lon_count - 1), (b + 1, lon_count - 2)) for b in range(lat_count - 1)]
    taken = {place for pair in pairs + routes for place in pair}
    masks = [mask for mask in (1, 3, 5, 4) if mask < lon_count]
    masks += [mask for mask in range(1, lon_count) if mask not in masks]
    for b in range(lat_count):
        for j in range(lon_count):
            if (b, j) not in taken:
                other = next((b, j ^ mask) for mask in masks if (b, j ^ mask) not in taken)
                taken |= {(b, j), other}
                pairs.append(((b, j), other))
    routes += pairs + [(t, s) for s, t in pairs]
    return [(s[1] * lat_count + s[0], t[1] * lat_count + t[0]) for s, t in routes]


def exchange(fields, bracket, fraction):
    count = lax.axis_size("lon")
    if count != SUBLANES:
        (payload,) = interpolate(fields, bracket, fraction, [count], None)
        received = lax.all_to_all(payload, "lon", split_axis=0, concat_axis=0, tiled=True)
        return [received], [(0, j, None) for j in range(count)]
    order = [0, 1] + [mask ^ 1 for mask in BEFORE]
    sizes = [1, 1 + len(BEFORE)]
    for mask in AFTER:
        order += [mask, mask ^ 1]
        sizes.append(2)
    for mask in BEFORE:
        order.append(mask)
        sizes.append(1)
    mine, other, *messages = interpolate(fields, bracket, fraction, sizes, order)
    other = swap(other, 1)
    blocks, parts = [mine, other], [(0, 0, 0), (1, 0, 1)]
    for mask, message in zip(AFTER, messages):
        message = swap(message, mask)
        blocks += [message, swap(message[1:], 1)]
        parts += [(len(blocks) - 2, 0, mask), (len(blocks) - 1, 0, mask ^ 1)]
    for i, (mask, message) in enumerate(zip(BEFORE, messages[len(AFTER) :])):
        blocks.append(swap(jnp.concatenate([message, other[i + 1 : i + 2]], 0), mask))
        parts += [(len(blocks) - 1, 0, mask), (len(blocks) - 1, 1, mask ^ 1)]
    return blocks, parts


def finish_kernel(own, meridional, zonal_out, meridional_out):
    variables, _, plev = zonal_out.shape
    for v in range(variables):
        zonal_out[v] = own[:, v * plev : (v + 1) * plev]
        meridional_out[v] = meridional[:, v * plev : (v + 1) * plev]


def finish(own, meridional, variables):
    out = jax.ShapeDtypeStruct((variables, 1, own.shape[0] // variables), f32)
    return pl.pallas_call(
        finish_kernel,
        out_shape=[out, out],
        in_specs=[VMEM] * 2,
        out_specs=[VMEM] * 2,
        compiler_params=pltpu.CompilerParams(vmem_limit_bytes=1 << 20),
        name="finish",
    )(own[None], meridional[None])


def shards(fields, bracket, fraction):
    variables, _, rows, columns = fields.shape
    plev = bracket.shape[0]
    pairs = variables * plev
    lon_count, lat_count = lax.axis_size("lon"), lax.axis_size("lat")
    lon_place, lat_place = lax.axis_index("lon"), lax.axis_index("lat")
    assert rows == lon_count

    blocks, parts = exchange(fields, bracket, fraction)

    if len(blocks) == 1:
        sums = jnp.sum(blocks[0][:, pairs:].astype(f32), 0)
    else:
        sums = sum(blocks[block][i, pairs:].astype(f32) for block, i, _ in parts)
    below, own, above, far = (sums[:4] + sums[4:]) / f32(lon_count * columns)
    first_place, last_place = lon_place == 0, lon_place == lon_count - 1

    beyond = lax.ppermute(far, ("lon", "lat"), edge_routes(lon_count, lat_count))

    on_pressure = lay(blocks, parts, pairs)

    below = jnp.where(first_place, beyond, below)
    above = jnp.where(last_place, beyond, above)
    first_row = first_place & (lat_place == 0)
    last_row = last_place & (lat_place == lat_count - 1)
    meridional = jnp.where(
        first_row, above - own, jnp.where(last_row, own - below, 0.5 * (above - below))
    )
    own, meridional = finish(own, meridional, variables)
    return (
        on_pressure.reshape(variables, plev, 1, lon_count * columns),
        own.reshape(variables, plev, 1),
        meridional.reshape(variables, plev, 1),
    )


def solution(mesh):
    return jax.shard_map(
        shards,
        mesh=mesh,
        in_specs=(P(None, None, "lat", "lon"), P(None, "lat", "lon"), P(None, "lat", "lon")),
        out_specs=(
            P(None, None, ("lat", "lon"), None),
            P(None, None, ("lat", "lon")),
            P(None, None, ("lat", "lon")),
        ),
        check_vma=False,
    )
```

```python
import functools

import jax
import jax.numpy as jnp
from jax import lax
from jax.experimental import pallas as pl
from jax.experimental.pallas import tpu as pltpu
from jax.sharding import PartitionSpec as P

WINDOW = 16
AFTER = (7,)
BEFORE = (5, 3)
SUBLANES = 8
CHUNKS = 4
PAD = 8
LIMIT = 8 << 20
bf16, f32 = jnp.bfloat16, jnp.float32
VMEM = pl.BlockSpec(memory_space=pltpu.VMEM)


def interpolate_kernel(fields, bracket, fraction, *refs, levels, order):
    *messages, flat, sums, near_fields, near_bracket, near_fraction, sem = refs
    places = [(message, i) for message in messages for i in range(message.shape[0])]
    groups, variables = fields.shape[:2]
    plev = bracket.shape[1]
    pairs = variables * plev
    step = levels // plev
    chunks = max(n for n in range(1, CHUNKS + 1) if (levels // 2) % n == 0)
    depth = levels // 2 // chunks

    def one_group(group):
        copies = [
            pltpu.make_async_copy(bracket.at[group], near_bracket.at[0], sem.at[chunks]),
            pltpu.make_async_copy(fraction.at[group], near_fraction.at[0], sem.at[chunks + 1]),
        ]
        copies += [
            pltpu.make_async_copy(
                fields.at[group, :, pl.ds(n * depth, depth)],
                near_fields.at[0, :, pl.ds(n * depth, depth)],
                sem.at[n],
            )
            for n in range(chunks)
        ]
        for copy in copies:
            copy.start()
        copies[0].wait()
        copies[1].wait()
        interpolate_group(group, copies[2:])

    def interpolate_group(group, arriving):
        for p in range(plev):
            base = min(p * step, levels - WINDOW)
            while arriving and (base + WINDOW) // 2 > depth * (chunks - len(arriving)):
                arriving.pop(0).wait()
            offset = near_bracket[0, p] - base
            index = jnp.concatenate([(offset + 1) >> 1, offset >> 1], 0).astype(f32).astype(bf16)
            high = index >= bf16(4)
            index = jnp.where(high, index - bf16(4), index)
            mid = index >= bf16(2)
            index = jnp.where(mid, index - bf16(2), index)
            low = index >= bf16(1)
            is_odd = (offset & 1) == 1
            weight = near_fraction[0, p].astype(f32)
            weight = jnp.where(is_odd, -weight, weight)
            for v in range(variables):
                w = [near_fields[0, v, base // 2 + k] for k in range(WINDOW // 2)]
                w = [jnp.where(low, w[k + 1], w[k]) for k in (0, 2, 4, 6)]
                w = [jnp.where(mid, w[k + 1], w[k]) for k in (0, 2)]
                picked = jnp.where(high, w[1], w[0]).astype(f32)
                even, odd = picked[:SUBLANES], picked[SUBLANES:]
                value = jnp.where(is_odd, odd, even) + weight * (odd - even)
                flat[pl.ds(v * plev + p, SUBLANES, stride=pairs + PAD), :] = value
        ones = jnp.ones((SUBLANES, flat.shape[1]), bf16)
        for r in range(SUBLANES):
            row = r
            if order:
                row = jnp.bitwise_xor(lax.axis_index("lon"), order[r])
            start = row * (pairs + PAD) if order is None else pl.multiple_of(row * (pairs + PAD), 8)
            block = flat[pl.ds(start, pairs), :].astype(bf16)
            if groups == 1:
                message, i = places[r]
                message[i, :pairs, :] = block
            else:
                messages[0][group * SUBLANES + r, :pairs, :] = block
            total = lax.dot_general(ones, block, (((1,), (1,)), ((), ())), preferred_element_type=f32)
            sums[pl.ds(SUBLANES * (group + 1) + row, 1), :] = total[:1]

    edge = jnp.zeros((SUBLANES, pairs), f32)
    sums[:SUBLANES, :] = edge
    sums[SUBLANES * (groups + 1) :, :] = edge
    if groups == 1:
        one_group(0)
    else:
        pl.loop(0, groups)(one_group)
    rows = groups * SUBLANES
    last, first = sums[rows + SUBLANES - 1 : rows + SUBLANES, :], sums[SUBLANES : SUBLANES + 1, :]
    place = lax.broadcasted_iota(jnp.int32, (SUBLANES, pairs), 0)
    for r, (message, i) in enumerate(places):
        row = r if order is None else jnp.bitwise_xor(lax.axis_index("lon"), order[r])
        three, again = sums[pl.ds(row + SUBLANES - 1, SUBLANES), :], sums[pl.ds(row + SUBLANES - 5, SUBLANES), :]
        four = jnp.where(place < 4, three, again)
        four = jnp.where((place & 3) == 3, jnp.where(2 * row < rows, last, first), four)
        main = four.astype(bf16).astype(f32)
        message[i, pairs:, :] = jnp.where(place < 4, main, four - main).astype(bf16)


def interpolate(fields, bracket, fraction, sizes, order):
    variables, levels, rows, columns = fields.shape
    plev = bracket.shape[0]
    groups = rows // SUBLANES
    pairs = variables * plev
    assert rows % SUBLANES == 0 and levels % 2 == 0 and pairs == columns
    grouped = fields.reshape(variables, levels, groups, SUBLANES, columns).transpose(2, 0, 1, 3, 4)
    grouped = grouped.reshape(groups, variables, levels // 2, 2 * SUBLANES, columns)
    bracket = bracket.reshape(plev, groups, SUBLANES, columns).transpose(1, 0, 2, 3)
    fraction = fraction.reshape(plev, groups, SUBLANES, columns).transpose(1, 0, 2, 3)
    return pl.pallas_call(
        functools.partial(interpolate_kernel, levels=levels, order=order),
        out_shape=[jax.ShapeDtypeStruct((n, pairs + SUBLANES, columns), bf16) for n in sizes],
        in_specs=[pl.BlockSpec(memory_space=pltpu.HBM)] * 3,
        out_specs=[VMEM] * len(sizes),
        scratch_shapes=[
            pltpu.VMEM((SUBLANES * (pairs + PAD), columns), f32),
            pltpu.VMEM((rows + 2 * SUBLANES, pairs), f32),
            pltpu.VMEM((1,) + grouped.shape[1:], bf16),
            pltpu.VMEM((1,) + bracket.shape[1:], jnp.int32),
            pltpu.VMEM((1,) + fraction.shape[1:], bf16),
            pltpu.SemaphoreType.DMA((CHUNKS + 2,)),
        ],
        compiler_params=pltpu.CompilerParams(vmem_limit_bytes=LIMIT),
        name="interpolate",
    )(*(pltpu.with_memory_space_constraint(x, pltpu.HBM) for x in (grouped, bracket, fraction)))


def lay_kernel(*refs, pairs, parts):
    *blocks, whole, sem = refs
    columns = blocks[0].shape[-1]
    copies = []
    for j, (block, i, mask) in enumerate(parts):
        source = j if mask is None else jnp.bitwise_xor(lax.axis_index("lon"), mask)
        start = pl.multiple_of(source * columns, columns)
        copies.append(
            pltpu.make_async_copy(
                blocks[block].at[i, :pairs], whole.at[:, pl.ds(start, columns)], sem.at[j]
            )
        )
    for copy in copies:
        copy.start()
    for copy in copies:
        copy.wait()


def lay(blocks, parts, pairs):
    columns = blocks[0].shape[-1]
    anywhere = pl.BlockSpec(memory_space=pl.ANY)
    return pl.pallas_call(
        functools.partial(lay_kernel, pairs=pairs, parts=parts),
        out_shape=jax.ShapeDtypeStruct((pairs, len(parts) * columns), bf16),
        in_specs=[anywhere] * len(blocks),
        out_specs=anywhere,
        scratch_shapes=[pltpu.SemaphoreType.DMA((len(parts),))],
        compiler_params=pltpu.CompilerParams(vmem_limit_bytes=1 << 20),
        cost_estimate=pl.CostEstimate(
            flops=2 * pairs * len(parts) * columns * 1024,
            bytes_accessed=4 * pairs * len(parts) * columns,
            transcendentals=0,
        ),
        name="lay",
    )(*blocks)


def swap(value, mask):
    return lax.ppermute(value, "lon", [(i, i ^ mask) for i in range(lax.axis_size("lon"))])


def edge_routes(lon_count, lat_count):
    routes, pairs = [], []
    if lon_count == 8 and lat_count > 1:
        top = lat_count - 1
        ring = [(0, 3)] + [(b, j) for b in range(1, lat_count) for j in (0, 1)] + [(top, 7), (top, 6)]
        ring += [(b, j) for b in reversed(range(top)) for j in (7, 6)] + [(0, 2)]
        routes += list(zip(ring, ring[1:] + ring[:1]))
    else:
        pairs += [((b, 0), (b - 1, 1)) for b in range(1, lat_count)]
        pairs += [((b, lon_count - 1), (b + 1, lon_count - 2)) for b in range(lat_count - 1)]
    taken = {place for pair in pairs + routes for place in pair}
    masks = [mask for mask in (1, 3, 5, 4) if mask < lon_count]
    masks += [mask for mask in range(1, lon_count) if mask not in masks]
    for b in range(lat_count):
        for j in range(lon_count):
            if (b, j) not in taken:
                other = next((b, j ^ mask) for mask in masks if (b, j ^ mask) not in taken)
                taken |= {(b, j), other}
                pairs.append(((b, j), other))
    routes += pairs + [(t, s) for s, t in pairs]
    return [(s[1] * lat_count + s[0], t[1] * lat_count + t[0]) for s, t in routes]


def exchange(fields, bracket, fraction):
    count = lax.axis_size("lon")
    if count != SUBLANES:
        (payload,) = interpolate(fields, bracket, fraction, [count], None)
        received = lax.all_to_all(payload, "lon", split_axis=0, concat_axis=0, tiled=True)
        return [received], [(0, j, None) for j in range(count)]
    order = [0, 1] + [mask ^ 1 for mask in BEFORE]
    sizes = [1, 1 + len(BEFORE)]
    for mask in AFTER:
        order += [mask, mask ^ 1]
        sizes.append(2)
    for mask in BEFORE:
        order.append(mask)
        sizes.append(1)
    mine, other, *messages = interpolate(fields, bracket, fraction, sizes, order)
    other = swap(other, 1)
    blocks, parts = [mine, other], [(0, 0, 0), (1, 0, 1)]
    for mask, message in zip(AFTER, messages):
        message = swap(message, mask)
        blocks += [message, swap(message[1:], 1)]
        parts += [(len(blocks) - 2, 0, mask), (len(blocks) - 1, 0, mask ^ 1)]
    for i, (mask, message) in enumerate(zip(BEFORE, messages[len(AFTER) :])):
        blocks.append(swap(jnp.concatenate([message, other[i + 1 : i + 2]], 0), mask))
        parts += [(len(blocks) - 1, 0, mask), (len(blocks) - 1, 1, mask ^ 1)]
    return blocks, parts


def finish_kernel(own, meridional, zonal_out, meridional_out, near_zonal, near_meridional, sem):
    variables, _, plev = zonal_out.shape
    copies = [
        pltpu.make_async_copy(near_zonal, zonal_out, sem.at[0]),
        pltpu.make_async_copy(near_meridional, meridional_out, sem.at[1]),
    ]
    for v in range(variables):
        near_zonal[v] = own[:, v * plev : (v + 1) * plev]
    copies[0].start()
    for v in range(variables):
        near_meridional[v] = meridional[:, v * plev : (v + 1) * plev]
    copies[1].start()
    for copy in copies:
        copy.wait()


def finish(own, meridional, variables):
    out = jax.ShapeDtypeStruct((variables, 1, own.shape[0] // variables), f32)
    return pl.pallas_call(
        finish_kernel,
        out_shape=[out, out],
        in_specs=[VMEM] * 2,
        out_specs=[pl.BlockSpec(memory_space=pl.ANY)] * 2,
        scratch_shapes=[
            pltpu.VMEM(out.shape, f32),
            pltpu.VMEM(out.shape, f32),
            pltpu.SemaphoreType.DMA((2,)),
        ],
        compiler_params=pltpu.CompilerParams(vmem_limit_bytes=1 << 20),
        name="finish",
    )(own[None], meridional[None])


def shards(fields, bracket, fraction):
    variables, _, rows, columns = fields.shape
    plev = bracket.shape[0]
    pairs = variables * plev
    lon_count, lat_count = lax.axis_size("lon"), lax.axis_size("lat")
    lon_place, lat_place = lax.axis_index("lon"), lax.axis_index("lat")
    assert rows == lon_count

    blocks, parts = exchange(fields, bracket, fraction)

    if len(blocks) == 1:
        sums = jnp.sum(blocks[0][:, pairs:].astype(f32), 0)
    else:
        sums = sum(blocks[block][i, pairs:].astype(f32) for block, i, _ in parts)
    below, own, above, far = (sums[:4] + sums[4:]) / f32(lon_count * columns)
    first_place, last_place = lon_place == 0, lon_place == lon_count - 1

    beyond = lax.ppermute(far, ("lon", "lat"), edge_routes(lon_count, lat_count))

    on_pressure = lay(blocks, parts, pairs)

    below = jnp.where(first_place, beyond, below)
    above = jnp.where(last_place, beyond, above)
    first_row = first_place & (lat_place == 0)
    last_row = last_place & (lat_place == lat_count - 1)
    meridional = jnp.where(
        first_row, above - own, jnp.where(last_row, own - below, 0.5 * (above - below))
    )
    own, meridional = finish(own, meridional, variables)
    return (
        on_pressure.reshape(variables, plev, 1, lon_count * columns),
        own.reshape(variables, plev, 1),
        meridional.reshape(variables, plev, 1),
    )


def solution(mesh):
    return jax.shard_map(
        shards,
        mesh=mesh,
        in_specs=(P(None, None, "lat", "lon"), P(None, "lat", "lon"), P(None, "lat", "lon")),
        out_specs=(
            P(None, None, ("lat", "lon"), None),
            P(None, None, ("lat", "lon")),
            P(None, None, ("lat", "lon")),
        ),
        check_vma=False,
    )
```
